128 devices in a mesh: row: 16 (over y_hi, z, core), col: 8 (over y_lo, x).
Axes of the slice: x: 4, y: 4 (y_hi: 2, y_lo: 2; y = y_hi * 2 + y_lo), z: 4, core: 2. Of those that a mesh axis runs over, the one named last changes fastest.
Arguments:
- vectors: float32 [49152, 128], P(('row', 'col')), may hold values from -6 to 6
- energies: float32 [49152], P(('row', 'col')), may hold values from 1 to 3
- intersections: bfloat16 [384, 512, 128], P(('row', 'col')), may hold values from -0.25 to 0.25
- coarse: bfloat16 [16, 16, 512, 512], P('col', 'row'), may hold values from -0.078125 to 0.078125
- fine_coarse: int32 [384], replicated, may hold values from 0 to 15, as said below
- coarse_slot: int32 [16], replicated, may hold values from 0 to 15, each once
- tile_codes: int32 [128, 432], P(('row', 'col')), may hold values from 0 to 1151, as said below
- tile_count: int32 [128], P(('row', 'col')), may hold values from 54 to 432, as said below
Outputs:
- first_step: float32 [49152, 128], P(('row', 'col'))
- second_step: float32 [49152, 128], P(('row', 'col'))
The draws below stay inside these ranges and needn't reach their ends.
Inputs may be any that keep to these rules, and one draw needn't show every extreme that they name: `fine_coarse`: fine block k lies on device d = k // 3; with c = d % (8) its coarse k-point lies in c * 2 to (c + 1) * 2 - 1. `coarse_slot`: each coarse k-point has its own position. `tile_codes`: each row lists distinct codes; a code e stands for output position e // (C 3) and input position e % (C 3) of the device's lists, with C = 8. Only the first tile_count[d] codes of row d are used; some device uses all 432.
All inputs are finite; a program needn't handle non-finite values.
Results may differ from the reference program's by a relative error of at most 0.0044.
Values may be sent and summed in bfloat16 or wider, within the bound.
A program may use at most 128 MiB of HBM per device.

```python
import jax
import jax.numpy as jnp
from jax import lax

TILE = 128
CP = 512
NV = 128
CKC = 2
BLK_DEV = 3
NB = 384
ORDER = 49152
NCK = 16
TILE_MAX = 432
N_ROW = 16
N_COL = 8
DEVICES = 128


def draw_fine_coarse(key, part):
    block_ids = jnp.arange(NB, dtype=jnp.int32)
    column = block_ids // BLK_DEV % (NCK // CKC)
    offsets = jax.random.randint(jax.random.fold_in(key, 7), (NB,), 0, CKC, dtype=jnp.int32)
    return (column * CKC + offsets).astype(jnp.int32)


def draw_tile_codes(key, part):
    device_keys = jax.random.split(jax.random.fold_in(key, 11), DEVICES)

    def draw_row(row_key):
        return jax.random.permutation(row_key, DEVICES * BLK_DEV * BLK_DEV)[:TILE_MAX].astype(jnp.int32)
    return jax.vmap(draw_row)(device_keys)


def draw_tile_count(key, part):
    count_key, pick_key = jax.random.split(jax.random.fold_in(key, 23))
    base = TILE_MAX // 8 + jax.random.randint(count_key, (DEVICES,), 0, TILE_MAX // 2 + 1, dtype=jnp.int32)
    busiest = jax.random.randint(pick_key, (), 0, DEVICES, dtype=jnp.int32)
    return jnp.where(jnp.arange(DEVICES, dtype=jnp.int32) == busiest, TILE_MAX, base).astype(jnp.int32)


def block_scale(own_key, dims, cuts, smallest, largest):
    loudness, own = 1.0, jax.random.fold_in(own_key, 6)
    for axis_at, parts in cuts:
        draws = jnp.exp(jax.random.uniform(jax.random.fold_in(own, axis_at), (parts,), jnp.float32, smallest / len(cuts), largest / len(cuts)))
        loudness = loudness * jnp.repeat(draws, dims[axis_at] // parts).reshape([-1 if axis == axis_at else 1 for axis in range(len(dims))])
    return loudness


def scatter_about(own_key, extent, deviation, reach, pieces=(), kind=jnp.bfloat16):
    level = block_scale(own_key, extent, pieces, -0.22, 0.18) if pieces else 1.0
    values = jax.random.normal(own_key, extent, jnp.float32) * deviation * level
    return jnp.minimum(jnp.maximum(values, -reach), reach).astype(kind)


def setup_inputs(seed: int = 0) -> dict:
    seeds = jax.random.split(jax.random.key(seed), 9)
    return {
        "vectors": scatter_about(seeds[0], (ORDER, NV), 1.0, 6.0, ((0, 128),), jnp.float32),
        "energies": jnp.clip(1.0 + 2.0 * jax.random.uniform(seeds[1], (ORDER,), jnp.float32) ** block_scale(seeds[1], (ORDER,), ((0, 128),), -0.2, 0.2), 1.0, 3.0),
        "intersections": scatter_about(seeds[2], (NB, CP, TILE), CP ** -0.5, 0.25, ((0, 128),)),
        "coarse": scatter_about(seeds[3], (NCK, NCK, CP, CP), (TILE * NB // 8) ** -0.5, 0.078125, ((0, 8), (1, 16))),
        "fine_coarse": draw_fine_coarse(jax.random.fold_in(seeds[8], 71), 0),
        "coarse_slot": jax.random.permutation(seeds[5], NCK).astype(jnp.int32),
        "tile_codes": draw_tile_codes(jax.random.fold_in(seeds[8], 71), 0),
        "tile_count": draw_tile_count(jax.random.fold_in(seeds[8], 71), 0),
    }


spectrum_center = 2.0
spectrum_half = 3.0


def device_part(device, rounded, intersections, coarse, fine_coarse, coarse_slot, tile_codes, tile_count):
    row_id = device // N_COL
    col_id = device % N_COL
    spread = N_COL * BLK_DEV
    index_out = jnp.arange(N_ROW * BLK_DEV, dtype=jnp.int32)
    index_in = jnp.arange(spread, dtype=jnp.int32)
    out_blocks = (((index_out // BLK_DEV) * N_COL + col_id) * BLK_DEV + index_out % BLK_DEV).astype(jnp.int32)
    in_blocks = ((row_id * N_COL + index_in // BLK_DEV) * BLK_DEV + index_in % BLK_DEV).astype(jnp.int32)
    own_points = (col_id * CKC + jnp.arange(CKC, dtype=jnp.int32)).astype(jnp.int32)
    in_slots = coarse_slot[fine_coarse[in_blocks]].astype(jnp.int32)
    blocks = coarse[own_points[:, None], in_slots[None, :]]
    over_in = intersections[in_blocks]
    projected = jnp.einsum("aicd,idt->aict", blocks.astype(jnp.float32), over_in.astype(jnp.float32)).astype(jnp.bfloat16)
    tile_list = tile_codes[device]
    out_idx = (tile_list // spread).astype(jnp.int32)
    in_idx = (tile_list % spread).astype(jnp.int32)
    out_block = out_blocks[out_idx]
    local_point = (fine_coarse[out_block] - col_id * CKC).astype(jnp.int32)
    right_sel = projected[local_point, in_idx]
    left_over = intersections[out_block]
    fine_tiles = jnp.einsum("kct,kcu->ktu", left_over.astype(jnp.float32), right_sel.astype(jnp.float32)).astype(jnp.bfloat16)
    live_mask = jnp.arange(TILE_MAX, dtype=jnp.int32) < tile_count[device]
    fine_tiles = jnp.where(live_mask[:, None, None], fine_tiles, jnp.zeros_like(fine_tiles))
    inputs = rounded[in_blocks[in_idx]]
    product = jnp.einsum("ktu,kun->ktn", fine_tiles.astype(jnp.float32), inputs.astype(jnp.float32))
    device_sum = jnp.zeros((N_ROW * BLK_DEV, TILE, NV), jnp.float32).at[out_idx].add(product)
    return out_blocks, device_sum


def apply_kernel(field, intersections, coarse, fine_coarse, coarse_slot, tile_codes, tile_count):
    rounded = field.astype(jnp.bfloat16)

    def visit(running, device):
        out_blocks, device_sum = device_part(device, rounded, intersections, coarse, fine_coarse, coarse_slot, tile_codes, tile_count)
        return running.at[out_blocks].add(device_sum), None

    result, _ = lax.scan(visit, jnp.zeros((NB, TILE, NV), jnp.float32), jnp.arange(DEVICES, dtype=jnp.int32))
    return result


def reference(vectors, energies, intersections, coarse, fine_coarse, coarse_slot, tile_codes, tile_count):
    start_vec = vectors.reshape(NB, TILE, NV)
    pair_energy = energies.reshape(NB, TILE, 1)

    def apply_shifted(field):
        kernel_part = apply_kernel(field, intersections, coarse, fine_coarse, coarse_slot, tile_codes, tile_count)
        return (pair_energy * field + kernel_part - spectrum_center * field) / spectrum_half

    first_step = apply_shifted(start_vec)
    second_step = 2.0 * apply_shifted(first_step) - start_vec
    return first_step.reshape(ORDER, NV), second_step.reshape(ORDER, NV)
```

```python
import functools

import jax
import jax.numpy as jnp
from jax import lax
from jax.experimental import pallas as pl
from jax.experimental.pallas import tpu as pltpu
from jax.sharding import PartitionSpec as P

spectrum_center = 2.0
spectrum_half = 3.0
chunk_pairs = 16
unroll_pairs = 4


def lookup(values_table, positions):
    matches = positions[:, None] == jnp.arange(values_table.shape[0], dtype=jnp.int32)[None, :]
    return jnp.sum(jnp.where(matches, values_table[None, :], 0), axis=1)


def pair_tables(codes, count, depth_out, spread, points, pairs_max):
    slots = jnp.arange(codes.shape[0], dtype=jnp.int32)
    all_codes = jnp.arange(depth_out * spread, dtype=jnp.int32)
    hits = (codes[:, None] == all_codes[None, :]) & (slots < count)[:, None]
    mask = jnp.any(hits, axis=0).astype(jnp.int32).reshape(depth_out, spread)
    filled = jnp.sum(mask, axis=1)
    pairs = (filled + 1) // 2
    index_out = jnp.arange(depth_out, dtype=jnp.int32)
    index_in = jnp.arange(spread, dtype=jnp.int32)
    base = jnp.sum(jnp.where(index_out[None, :] < index_out[:, None], pairs[None, :], 0), axis=1)
    rank = jnp.sum(
        jnp.where(index_in[None, None, :] < index_in[None, :, None], mask[:, None, :], 0), axis=2
    )
    place = jnp.where(mask > 0, 2 * base[:, None] + rank, -1).reshape(-1)
    spots = jnp.arange(2 * pairs_max, dtype=jnp.int32)
    found = jnp.sum(
        jnp.where(spots[:, None] == place[None, :], all_codes[None, :] + 1, 0), axis=1
    )
    found = found.reshape(pairs_max, 2)
    live = found > 0
    code = jnp.maximum(found - 1, 0)
    out_idx = jnp.where(live[:, 0], code[:, 0] // spread, depth_out - 1)
    in_idx = jnp.where(live, code % spread, spread)
    point = lookup(points, out_idx)
    return out_idx, in_idx[:, 0], in_idx[:, 1], point, jnp.sum(pairs).reshape(1)


def add_pair(total_ref, fields_ref, tile, block, first, second):
    both = jnp.concatenate([fields_ref[first], fields_ref[second]], axis=0)
    return total_ref, block, jnp.dot(tile, both, preferred_element_type=jnp.float32)


def build_kernel(
    spread,
    slots_ref,
    out_ref_idx,
    first_idx,
    second_idx,
    point_idx,
    used_ref,
    coarse_ref,
    over_in_ref,
    over_out_ref,
    fields_ref,
    tiles_ref,
    partial_ref,
    projected_ref,
    total_ref,
):
    step = pl.program_id(0)
    points = coarse_ref.shape[0]

    @pl.when(step == 0)
    def _():
        total_ref[...] = jnp.zeros_like(total_ref)

    @pl.when(step < spread)
    def _():
        for a in range(points):
            projected_ref[step * points + a] = jnp.dot(
                coarse_ref[a, 0], over_in_ref[0], preferred_element_type=jnp.float32
            ).astype(jnp.bfloat16)

    start = (step - spread) * chunk_pairs

    @pl.when((step >= spread) & (start < used_ref[0]))
    def _():
        def group(g, carry):
            adds = []
            for k in range(unroll_pairs):
                local = g * unroll_pairs + k
                pair = start + local
                block, first, second = out_ref_idx[pair], first_idx[pair], second_idx[pair]
                a = point_idx[pair]
                left = jnp.minimum(first, spread - 1) * points + a
                right = jnp.minimum(second, spread - 1) * points + a
                both = jnp.concatenate([projected_ref[left], projected_ref[right]], axis=1)
                tile = jnp.dot(
                    over_out_ref[block], both, preferred_element_type=jnp.float32
                ).astype(jnp.bfloat16)
                tiles_ref[local] = tile
                adds.append(add_pair(total_ref, fields_ref, tile, block, first, second))
            for ref, block, product in adds:
                ref[block] += product
            return carry

        lax.fori_loop(0, chunk_pairs // unroll_pairs, group, 0)

    @pl.when(step == pl.num_programs(0) - 1)
    def _():
        partial_ref[...] = total_ref[...].astype(partial_ref.dtype)


def apply_kernel_body(
    out_ref_idx, first_idx, second_idx, used_ref, tiles_ref, fields_ref, partial_ref, total_ref
):
    step = pl.program_id(0)

    @pl.when(step == 0)
    def _():
        total_ref[...] = jnp.zeros_like(total_ref)

    start = step * chunk_pairs

    @pl.when(start < used_ref[0])
    def _():
        def group(g, carry):
            adds = []
            for k in range(unroll_pairs):
                local = g * unroll_pairs + k
                pair = start + local
                adds.append(
                    add_pair(
                        total_ref,
                        fields_ref,
                        tiles_ref[local],
                        out_ref_idx[pair],
                        first_idx[pair],
                        second_idx[pair],
                    )
                )
            for ref, block, product in adds:
                ref[block] += product
            return carry

        lax.fori_loop(0, chunk_pairs // unroll_pairs, group, 0)

    @pl.when(step == pl.num_programs(0) - 1)
    def _():
        partial_ref[...] = total_ref[...].astype(partial_ref.dtype)


def build_tiles(in_slots, tables, coarse_strip, over_in, over_out, fields, pairs_max):
    points, _, pairs_coarse, _ = coarse_strip.shape
    spread = over_in.shape[0]
    depth_out, tile_side, _ = over_out.shape
    width = fields.shape[2]
    chunks = pairs_max // chunk_pairs

    def tile_chunk(s, *refs):
        last = jnp.maximum((refs[5][0] + chunk_pairs - 1) // chunk_pairs - 1, 0)
        return (jnp.clip(s - spread, 0, last), 0, 0)

    def held(s, *refs):
        return (0, 0, 0)

    grid_spec = pltpu.PrefetchScalarGridSpec(
        num_scalar_prefetch=6,
        grid=(spread + chunks,),
        in_specs=[
            pl.BlockSpec(
                (points, 1, pairs_coarse, pairs_coarse),
                lambda s, slots, *refs: (0, slots[jnp.minimum(s, spread - 1)], 0, 0),
            ),
            pl.BlockSpec(
                (1, pairs_coarse, tile_side), lambda s, *refs: (jnp.minimum(s, spread - 1), 0, 0)
            ),
            pl.BlockSpec(over_out.shape, held),
            pl.BlockSpec(fields.shape, held),
        ],
        out_specs=[
            pl.BlockSpec((chunk_pairs, tile_side, 2 * tile_side), tile_chunk),
            pl.BlockSpec((depth_out, tile_side, width), held),
        ],
        scratch_shapes=[
            pltpu.VMEM((spread * points, pairs_coarse, tile_side), jnp.bfloat16),
            pltpu.VMEM((depth_out, tile_side, width), jnp.float32),
        ],
    )
    return pl.pallas_call(
        functools.partial(build_kernel, spread),
        grid_spec=grid_spec,
        out_shape=[
            jax.ShapeDtypeStruct((pairs_max, tile_side, 2 * tile_side), jnp.bfloat16),
            jax.ShapeDtypeStruct((depth_out, tile_side, width), jnp.bfloat16),
        ],
        compiler_params=pltpu.CompilerParams(vmem_limit_bytes=52 * 1024 * 1024),
        name="build_tiles",
    )(in_slots, *tables, coarse_strip, over_in, over_out, fields)


def apply_tiles(tables, tiles, fields, depth_out):
    pairs_max, tile_side, _ = tiles.shape
    width = fields.shape[2]
    out_idx, first, second, _, used = tables

    def tile_chunk(s, *refs):
        last = jnp.maximum((refs[3][0] + chunk_pairs - 1) // chunk_pairs - 1, 0)
        return (jnp.minimum(s, last), 0, 0)

    def held(s, *refs):
        return (0, 0, 0)

    grid_spec = pltpu.PrefetchScalarGridSpec(
        num_scalar_prefetch=4,
        grid=(pairs_max // chunk_pairs,),
        in_specs=[
            pl.BlockSpec((chunk_pairs, tile_side, 2 * tile_side), tile_chunk),
            pl.BlockSpec(fields.shape, held),
        ],
        out_specs=pl.BlockSpec((depth_out, tile_side, width), held),
        scratch_shapes=[pltpu.VMEM((depth_out, tile_side, width), jnp.float32)],
    )
    return pl.pallas_call(
        apply_kernel_body,
        grid_spec=grid_spec,
        out_shape=jax.ShapeDtypeStruct((depth_out, tile_side, width), jnp.bfloat16),
        compiler_params=pltpu.CompilerParams(vmem_limit_bytes=32 * 1024 * 1024),
        name="apply_tiles",
    )(out_idx, first, second, used, tiles, fields)


def on_device(
    vectors, energies, intersections, coarse, fine_coarse, coarse_slot, tile_codes, tile_count
):
    rows_count = lax.axis_size("row")
    cols_count = lax.axis_size("col")
    row_id = lax.axis_index("row")
    col_id = lax.axis_index("col")
    blocks_dev, pairs_coarse, tile_side = intersections.shape
    width_vec = vectors.shape[1]
    points_col = coarse.shape[0]
    spread = cols_count * blocks_dev
    depth_out = rows_count * blocks_dev
    pairs_max = (tile_codes.shape[1] + depth_out) // 2
    pairs_max = -(-pairs_max // chunk_pairs) * chunk_pairs
    index_out = jnp.arange(depth_out, dtype=jnp.int32)
    index_in = jnp.arange(spread, dtype=jnp.int32)
    out_blocks = (
        index_out // blocks_dev * cols_count + col_id
    ) * blocks_dev + index_out % blocks_dev
    in_blocks = (row_id * cols_count + index_in // blocks_dev) * blocks_dev + index_in % blocks_dev
    in_slots = lookup(coarse_slot, lookup(fine_coarse, in_blocks))
    out_points = lookup(fine_coarse, out_blocks) - col_id * points_col
    tables = pair_tables(
        tile_codes[0], tile_count[0], depth_out, spread, out_points, pairs_max
    )

    coarse_strip = lax.all_gather(coarse, "row", axis=1, tiled=True)
    over_in = lax.all_gather(intersections, "col", axis=0, tiled=True)
    over_out = lax.all_gather(jnp.swapaxes(intersections, 1, 2), "row", axis=0, tiled=True)

    def gathered(field):
        rounded = field.astype(jnp.bfloat16)
        copies = jnp.broadcast_to(rounded, (cols_count, *rounded.shape))
        pieces = lax.all_to_all(copies, "col", split_axis=0, concat_axis=0, tiled=True)
        pieces = pieces.reshape(spread, tile_side, width_vec)
        return jnp.pad(pieces, ((0, 1), (0, 0), (0, 0)))

    def summed(partial):
        parts = partial.reshape(rows_count, blocks_dev, tile_side, width_vec)
        arrived = lax.all_to_all(parts, "row", split_axis=0, concat_axis=0, tiled=True)
        return jnp.sum(arrived.astype(jnp.float32), axis=0)

    start_vec = vectors.reshape(blocks_dev, tile_side, width_vec)
    pair_energy = energies.reshape(blocks_dev, tile_side, 1)

    def shifted(field, kernel_part):
        return (pair_energy * field + kernel_part - spectrum_center * field) / spectrum_half

    tiles, partial = build_tiles(
        in_slots, tables, coarse_strip, over_in, over_out, gathered(start_vec), pairs_max
    )
    first_step = shifted(start_vec, summed(partial))
    partial = apply_tiles(tables, tiles, gathered(first_step), depth_out)
    second_step = 2.0 * shifted(first_step, summed(partial)) - start_vec
    return (
        first_step.reshape(blocks_dev * tile_side, width_vec),
        second_step.reshape(blocks_dev * tile_side, width_vec),
    )


def solution(mesh):
    in_specs = (
        P(("row", "col"), None),
        P(("row", "col")),
        P(("row", "col"), None, None),
        P("col", "row", None, None),
        P(),
        P(),
        P(("row", "col"), None),
        P(("row", "col")),
    )
    out_specs = (P(("row", "col"), None), P(("row", "col"), None))
    return jax.shard_map(
        on_device, mesh=mesh, in_specs=in_specs, out_specs=out_specs, check_vma=False
    )
```

```python
import functools

import jax
import jax.numpy as jnp
from jax import lax
from jax.experimental import pallas as pl
from jax.experimental.pallas import tpu as pltpu
from jax.sharding import PartitionSpec as P

spectrum_center = 2.0
spectrum_half = 3.0
chunk_pairs = 16
unroll_pairs = 4
gather_copies = 53
MESH = pl.DeviceIdType.MESH


def lookup(values_table, positions):
    matches = positions[:, None] == jnp.arange(values_table.shape[0], dtype=jnp.int32)[None, :]
    return jnp.sum(jnp.where(matches, values_table[None, :], 0), axis=1)


def pair_tables(codes, count, depth_out, spread, points, pairs_max):
    slots = jnp.arange(codes.shape[0], dtype=jnp.int32)
    all_codes = jnp.arange(depth_out * spread, dtype=jnp.int32)
    hits = (codes[:, None] == all_codes[None, :]) & (slots < count)[:, None]
    mask = jnp.any(hits, axis=0).astype(jnp.int32).reshape(depth_out, spread)
    filled = jnp.sum(mask, axis=1)
    pairs = (filled + 1) // 2
    index_out = jnp.arange(depth_out, dtype=jnp.int32)
    index_in = jnp.arange(spread, dtype=jnp.int32)
    base = jnp.sum(jnp.where(index_out[None, :] < index_out[:, None], pairs[None, :], 0), axis=1)
    rank = jnp.sum(
        jnp.where(index_in[None, None, :] < index_in[None, :, None], mask[:, None, :], 0), axis=2
    )
    place = jnp.where(mask > 0, 2 * base[:, None] + rank, -1).reshape(-1)
    spots = jnp.arange(2 * pairs_max, dtype=jnp.int32)
    found = jnp.sum(
        jnp.where(spots[:, None] == place[None, :], all_codes[None, :] + 1, 0), axis=1
    )
    found = found.reshape(pairs_max, 2)
    live = found > 0
    code = jnp.maximum(found - 1, 0)
    out_idx = jnp.where(live[:, 0], code[:, 0] // spread, depth_out - 1)
    in_idx = jnp.where(live, code % spread, spread)
    point = lookup(points, out_idx)
    return out_idx, in_idx[:, 0], in_idx[:, 1], point, jnp.sum(pairs).reshape(1)


def block_of(ref, block, blocks_dev, side):
    rows = pl.ds(pl.multiple_of(block % blocks_dev * side, side), side)
    return ref[block // blocks_dev, rows, :]


def add_pair(total_ref, fields_ref, tile, block, first, second):
    blocks_dev = fields_ref.shape[1] // total_ref.shape[1]
    side = total_ref.shape[1]
    both = jnp.concatenate(
        [block_of(fields_ref, place, blocks_dev, side) for place in (first, second)], axis=0
    )
    return total_ref, block, jnp.dot(tile, both, preferred_element_type=jnp.float32)


def build_kernel(
    blocks_dev,
    spread,
    slots_ref,
    out_ref_idx,
    first_idx,
    second_idx,
    point_idx,
    used_ref,
    coarse_a_ref,
    coarse_b_ref,
    over_in_ref,
    packed_a_ref,
    packed_i_ref,
    tiles_ref,
    partial_ref,
    projected_ref,
    total_ref,
    over_out_ref,
    fields_ref,
    sems,
):
    step = pl.program_id(0)
    side = total_ref.shape[1]
    depth = coarse_a_ref.shape[1]
    cols = packed_i_ref.shape[0]
    copies = (
        pltpu.make_async_copy(
            packed_a_ref.at[:, pl.ds(depth, blocks_dev * side), :], over_out_ref, sems.at[0]
        ),
        pltpu.make_async_copy(
            packed_i_ref.at[:, pl.ds(blocks_dev * depth, blocks_dev * side), :],
            fields_ref.at[pl.ds(0, cols)],
            sems.at[1],
        ),
    )

    @pl.when(step == 0)
    def _():
        for copy in copies:
            copy.start()
        total_ref[...] = jnp.zeros_like(total_ref)
        fields_ref[cols] = jnp.zeros(fields_ref.shape[1:], fields_ref.dtype)

    @pl.when(step < spread)
    def _():
        for a, ref in enumerate((coarse_a_ref, coarse_b_ref)):
            projected_ref[step * 2 + a] = jnp.dot(
                ref[0], over_in_ref[0], preferred_element_type=jnp.float32
            ).astype(jnp.bfloat16)

    @pl.when(step == spread)
    def _():
        for copy in copies:
            copy.wait()

    start = (step - spread) * chunk_pairs

    @pl.when((step >= spread) & (start < used_ref[0]))
    def _():
        def group(g, carry):
            adds = []
            for k in range(unroll_pairs):
                local = g * unroll_pairs + k
                pair = start + local
                block, first, second = out_ref_idx[pair], first_idx[pair], second_idx[pair]
                a = point_idx[pair]
                left = jnp.minimum(first, spread - 1) * 2 + a
                right = jnp.minimum(second, spread - 1) * 2 + a
                both = jnp.concatenate([projected_ref[left], projected_ref[right]], axis=1)
                tile = jnp.dot(
                    block_of(over_out_ref, block, blocks_dev, side),
                    both,
                    preferred_element_type=jnp.float32,
                ).astype(jnp.bfloat16)
                tiles_ref[local] = tile
                adds.append(add_pair(total_ref, fields_ref, tile, block, first, second))
            for ref, block, product in adds:
                ref[block] += product
            return carry

        lax.fori_loop(0, chunk_pairs // unroll_pairs, group, 0)

    @pl.when(step == pl.num_programs(0) - 1)
    def _():
        partial_ref[...] = total_ref[...].astype(partial_ref.dtype)


def apply_kernel_body(
    out_ref_idx,
    first_idx,
    second_idx,
    used_ref,
    tiles_ref,
    pieces_ref,
    partial_ref,
    total_ref,
    fields_ref,
):
    step = pl.program_id(0)
    cols = pieces_ref.shape[0]

    @pl.when(step == 0)
    def _():
        total_ref[...] = jnp.zeros_like(total_ref)
        fields_ref[pl.ds(0, cols)] = pieces_ref[...]
        fields_ref[cols] = jnp.zeros(fields_ref.shape[1:], fields_ref.dtype)

    start = step * chunk_pairs

    @pl.when(start < used_ref[0])
    def _():
        def group(g, carry):
            adds = []
            for k in range(unroll_pairs):
                local = g * unroll_pairs + k
                pair = start + local
                adds.append(
                    add_pair(
                        total_ref,
                        fields_ref,
                        tiles_ref[local],
                        out_ref_idx[pair],
                        first_idx[pair],
                        second_idx[pair],
                    )
                )
            for ref, block, product in adds:
                ref[block] += product
            return carry

        lax.fori_loop(0, chunk_pairs // unroll_pairs, group, 0)

    @pl.when(step == pl.num_programs(0) - 1)
    def _():
        partial_ref[...] = total_ref[...].astype(partial_ref.dtype)


def gather_kernel(a_ref, b_ref, i_ref, out_a, out_b, out_i, send_sem, recv_sem, own_sem):
    row, col = lax.axis_index("row"), lax.axis_index("col")
    h, z, k = row // 8, row // 2 % 4, row % 2
    l, x = col // 4, col % 4

    def row_of(hh, zz):
        return (hh * 4 + zz % 4) * 2 + k

    partner = (row_of(1 - h, z), col)
    z_dev = ((row_of(h, z + 1), col), (row_of(h, z + 3), col))
    x_dev = ((row, l * 4 + (x + 1) % 4), (row, l * 4 + (x + 3) % 4))
    sibling = (row + 1 - 2 * k, col)
    pair = (row, (1 - l) * 4 + x)

    barrier = pltpu.get_barrier_semaphore()
    neighbours = (partner, *z_dev, *x_dev, sibling, pair)
    for device in neighbours:
        pl.semaphore_signal(barrier, inc=1, device_id=device, device_id_type=MESH)
    pl.semaphore_wait(barrier, len(neighbours))

    def halves(ref):
        size = ref.shape[0] // 2
        return [pl.ds(s * size, size) for s in range(2)]

    half_a, half_b, half_i = halves(a_ref), halves(b_ref), halves(i_ref)
    copies, to_sibling = [], []

    def send(src, dst, device):
        copy = pltpu.make_async_remote_copy(
            src_ref=src,
            dst_ref=dst,
            send_sem=send_sem.at[len(copies)],
            recv_sem=recv_sem.at[len(copies)],
            device_id=device,
            device_id_type=MESH,
        )
        copy.start()
        copies.append(copy)
        return copy

    def pass_on(out, slot, part, device):
        return send(out.at[slot, part], out.at[slot, part], device)

    def share(out, slot):
        to_sibling.append(send(out.at[slot], out.at[slot], sibling))

    def forward(arrivals, out, slots, parts, devices):
        sent = []
        for d in range(2):
            arrivals[d][d].wait_recv()
            sent.append(pass_on(out, slots[d], parts[d], devices[d]))
        arrivals[0][1].wait_recv()
        arrivals[1][0].wait_recv()
        return sent

    a_y = [send(a_ref.at[p], out_a.at[row, p], partner) for p in half_a]
    b_z = [[send(b_ref.at[p], out_b.at[row, p], z_dev[d]) for p in half_b] for d in range(2)]
    i_x = [[send(i_ref.at[p], out_i.at[col, p], x_dev[d]) for p in half_i] for d in range(2)]
    to_sibling.append(send(a_ref, out_a.at[row], sibling))
    to_sibling.append(send(b_ref, out_b.at[row], sibling))
    own = [
        pltpu.make_async_copy(a_ref, out_a.at[row], own_sem.at[0]),
        pltpu.make_async_copy(b_ref, out_b.at[row], own_sem.at[1]),
        pltpu.make_async_copy(i_ref, out_i.at[col], own_sem.at[2]),
    ]
    for copy in own:
        copy.start()

    z_rows = (row_of(h, z + 3), row_of(h, z + 1))
    far = row_of(h, z + 2)
    x_cols = (l * 4 + (x + 3) % 4, l * 4 + (x + 1) % 4)
    other = row_of(1 - h, z)
    other_rows = (row_of(1 - h, z + 3), row_of(1 - h, z + 1))
    other_far = row_of(1 - h, z + 2)
    pair_col = (1 - l) * 4 + x
    other_cols = ((1 - l) * 4 + (x + 3) % 4, (1 - l) * 4 + (x + 1) % 4)

    b_zf = forward(b_z, out_b, z_rows, half_b, z_dev)
    a_z = [[send(a_ref.at[p], out_a.at[row, p], z_dev[d]) for p in half_a] for d in range(2)]
    for slot in z_rows:
        share(out_b, slot)
    a2_z = [[None, None], [None, None]]
    for s in range(2):
        a_y[s].wait_recv()
        for d in range(2):
            a2_z[d][s] = pass_on(out_a, other, half_a[s], z_dev[d])
    share(out_a, other)
    i_pair = send(i_ref, out_i.at[col], pair)
    b_y = [send(b_ref, out_b.at[row], partner)]
    for slot in z_rows:
        b_y.append(send(out_b.at[slot], out_b.at[slot], partner))
    i_xf = forward(i_x, out_i, x_cols, half_i, x_dev)
    for d in range(2):
        b_zf[d].wait_recv()
    b_y.append(send(out_b.at[far], out_b.at[far], partner))
    share(out_b, far)
    a_zf = forward(a_z, out_a, z_rows, half_a, z_dev)
    for slot in z_rows:
        share(out_a, slot)
    i_pair.wait_recv()
    i2_x = [[pass_on(out_i, pair_col, p, x_dev[d]) for p in half_i] for d in range(2)]
    for d in range(2):
        a_zf[d].wait_recv()
    share(out_a, far)
    i2_xf = forward(i2_x, out_i, other_cols, half_i, x_dev)
    a2_zf = forward(a2_z, out_a, other_rows, half_a, z_dev)
    for slot in other_rows:
        share(out_a, slot)
    for slot, copy in zip((other, *other_rows, other_far), b_y):
        copy.wait_recv()
        share(out_b, slot)
    for d in range(2):
        a2_zf[d].wait_recv()
    share(out_a, other_far)
    for copy in (*i_xf, *i2_xf, *to_sibling):
        copy.wait_recv()
    for copy in own:
        copy.wait()
    assert len(copies) == gather_copies
    for copy in copies:
        copy.wait_send()


def gather_all(a, b, i):
    rows, cols = lax.axis_size("row"), lax.axis_size("col")
    vmem = pl.BlockSpec(memory_space=pltpu.VMEM)
    anywhere = pl.BlockSpec(memory_space=pl.ANY)
    return pl.pallas_call(
        gather_kernel,
        in_specs=[vmem, vmem, vmem],
        out_specs=[anywhere] * 3,
        out_shape=[
            jax.ShapeDtypeStruct((rows, *a.shape), a.dtype),
            jax.ShapeDtypeStruct((rows, *b.shape), b.dtype),
            jax.ShapeDtypeStruct((cols, *i.shape), i.dtype),
        ],
        scratch_shapes=[
            pltpu.SemaphoreType.DMA((gather_copies,)),
            pltpu.SemaphoreType.DMA((gather_copies,)),
            pltpu.SemaphoreType.DMA((3,)),
        ],
        compiler_params=pltpu.CompilerParams(collective_id=0, has_side_effects=True),
        name="gather_all",
    )(a, b, i)


def build_tiles(in_slots, tables, packed_a, packed_b, packed_i, pairs_max, blocks_dev, side):
    rows, cols = packed_a.shape[0], packed_i.shape[0]
    depth = packed_b.shape[1]
    width = packed_i.shape[2]
    spread, depth_out = cols * blocks_dev, rows * blocks_dev
    chunks = pairs_max // chunk_pairs

    def tile_chunk(s, *refs):
        last = jnp.maximum((refs[5][0] + chunk_pairs - 1) // chunk_pairs - 1, 0)
        return (jnp.clip(s - spread, 0, last), 0, 0)

    def coarse_at(s, slots, *refs):
        return (slots[jnp.minimum(s, spread - 1)], 0, 0)

    def over_in_at(s, *refs):
        block = jnp.minimum(s, spread - 1)
        return (block // blocks_dev, block % blocks_dev, 0)

    grid_spec = pltpu.PrefetchScalarGridSpec(
        num_scalar_prefetch=6,
        grid=(spread + chunks,),
        in_specs=[
            pl.BlockSpec((1, depth, depth), coarse_at),
            pl.BlockSpec((1, depth, depth), coarse_at),
            pl.BlockSpec((1, depth, side), over_in_at),
            pl.BlockSpec(memory_space=pl.ANY),
            pl.BlockSpec(memory_space=pl.ANY),
        ],
        out_specs=[
            pl.BlockSpec((chunk_pairs, side, 2 * side), tile_chunk),
            pl.BlockSpec((depth_out, side, width), lambda s, *refs: (0, 0, 0)),
        ],
        scratch_shapes=[
            pltpu.VMEM((spread * 2, depth, side), jnp.bfloat16),
            pltpu.VMEM((depth_out, side, width), jnp.float32),
            pltpu.VMEM((rows, blocks_dev * side, depth), jnp.bfloat16),
            pltpu.VMEM((cols + 1, blocks_dev * side, width), jnp.bfloat16),
            pltpu.SemaphoreType.DMA((2,)),
        ],
    )
    return pl.pallas_call(
        functools.partial(build_kernel, blocks_dev, spread),
        grid_spec=grid_spec,
        out_shape=[
            jax.ShapeDtypeStruct((pairs_max, side, 2 * side), jnp.bfloat16),
            jax.ShapeDtypeStruct((depth_out, side, width), jnp.bfloat16),
        ],
        compiler_params=pltpu.CompilerParams(vmem_limit_bytes=40 * 1024 * 1024),
        name="build_tiles",
    )(in_slots, *tables, packed_a, packed_b, packed_i, packed_a, packed_i)


def apply_tiles(tables, tiles, pieces, depth_out):
    pairs_max, side, _ = tiles.shape
    cols, rows_dev, width = pieces.shape
    out_idx, first, second, _, used = tables

    def tile_chunk(s, *refs):
        last = jnp.maximum((refs[3][0] + chunk_pairs - 1) // chunk_pairs - 1, 0)
        return (jnp.minimum(s, last), 0, 0)

    def held(s, *refs):
        return (0, 0, 0)

    grid_spec = pltpu.PrefetchScalarGridSpec(
        num_scalar_prefetch=4,
        grid=(pairs_max // chunk_pairs,),
        in_specs=[
            pl.BlockSpec((chunk_pairs, side, 2 * side), tile_chunk),
            pl.BlockSpec(pieces.shape, held),
        ],
        out_specs=pl.BlockSpec((depth_out, side, width), held),
        scratch_shapes=[
            pltpu.VMEM((depth_out, side, width), jnp.float32),
            pltpu.VMEM((cols + 1, rows_dev, width), jnp.bfloat16),
        ],
    )
    return pl.pallas_call(
        apply_kernel_body,
        grid_spec=grid_spec,
        out_shape=jax.ShapeDtypeStruct((depth_out, side, width), jnp.bfloat16),
        compiler_params=pltpu.CompilerParams(vmem_limit_bytes=32 * 1024 * 1024),
        name="apply_tiles",
    )(out_idx, first, second, used, tiles, pieces)


def on_device(
    vectors, energies, intersections, coarse, fine_coarse, coarse_slot, tile_codes, tile_count
):
    rows_count = lax.axis_size("row")
    cols_count = lax.axis_size("col")
    row_id = lax.axis_index("row")
    col_id = lax.axis_index("col")
    blocks_dev, pairs_coarse, tile_side = intersections.shape
    width_vec = vectors.shape[1]
    points_col = coarse.shape[0]
    spread = cols_count * blocks_dev
    depth_out = rows_count * blocks_dev
    pairs_max = (tile_codes.shape[1] + depth_out) // 2
    pairs_max = -(-pairs_max // chunk_pairs) * chunk_pairs
    index_out = jnp.arange(depth_out, dtype=jnp.int32)
    index_in = jnp.arange(spread, dtype=jnp.int32)
    out_blocks = (
        index_out // blocks_dev * cols_count + col_id
    ) * blocks_dev + index_out % blocks_dev
    in_blocks = (row_id * cols_count + index_in // blocks_dev) * blocks_dev + index_in % blocks_dev
    in_slots = lookup(coarse_slot, lookup(fine_coarse, in_blocks))
    out_points = lookup(fine_coarse, out_blocks) - col_id * points_col
    tables = pair_tables(
        tile_codes[0], tile_count[0], depth_out, spread, out_points, pairs_max
    )

    start_vec = vectors.reshape(blocks_dev, tile_side, width_vec)
    pair_energy = energies.reshape(blocks_dev, tile_side, 1)
    across = jnp.swapaxes(intersections, 1, 2).reshape(-1, pairs_coarse)
    packed_a, packed_b, packed_i = gather_all(
        jnp.concatenate([coarse[0, 0], across], axis=0),
        coarse[1, 0],
        jnp.concatenate(
            [intersections.reshape(-1, tile_side), vectors.astype(jnp.bfloat16)], axis=0
        ),
    )

    def summed(partial):
        parts = partial.reshape(rows_count, blocks_dev, tile_side, width_vec)
        arrived = lax.all_to_all(parts, "row", split_axis=0, concat_axis=0, tiled=True)
        return jnp.sum(arrived.astype(jnp.float32), axis=0)

    def shifted(field, kernel_part):
        return (pair_energy * field + kernel_part - spectrum_center * field) / spectrum_half

    tiles, partial = build_tiles(
        in_slots, tables, packed_a, packed_b, packed_i, pairs_max, blocks_dev, tile_side
    )
    first_step = shifted(start_vec, summed(partial))
    rounded = first_step.astype(jnp.bfloat16).reshape(1, blocks_dev * tile_side, width_vec)
    pieces = lax.all_to_all(
        jnp.broadcast_to(rounded, (cols_count, *rounded.shape[1:])),
        "col",
        split_axis=0,
        concat_axis=0,
        tiled=True,
    )
    partial = apply_tiles(tables, tiles, pieces, depth_out)
    second_step = 2.0 * shifted(first_step, summed(partial)) - start_vec
    return (
        first_step.reshape(blocks_dev * tile_side, width_vec),
        second_step.reshape(blocks_dev * tile_side, width_vec),
    )


def solution(mesh):
    in_specs = (
        P(("row", "col"), None),
        P(("row", "col")),
        P(("row", "col"), None, None),
        P("col", "row", None, None),
        P(),
        P(),
        P(("row", "col"), None),
        P(("row", "col")),
    )
    out_specs = (P(("row", "col"), None), P(("row", "col"), None))
    return jax.shard_map(
        on_device, mesh=mesh, in_specs=in_specs, out_specs=out_specs, check_vma=False
    )
```

```python
import functools

import jax
import jax.numpy as jnp
from jax import lax
from jax.experimental import pallas as pl
from jax.experimental.pallas import tpu as pltpu
from jax.sharding import PartitionSpec as P

spectrum_center = 2.0
spectrum_half = 3.0
chunk_pairs = 16
unroll_pairs = 8
gather_copies = 53
block_parts = 3
MESH = pl.DeviceIdType.MESH


def lookup(values_table, positions):
    matches = positions[:, None] == jnp.arange(values_table.shape[0], dtype=jnp.int32)[None, :]
    return jnp.sum(jnp.where(matches, values_table[None, :], 0), axis=1)


def pair_tables(codes, count, depth_out, spread, points, pairs_max):
    slots = jnp.arange(codes.shape[0], dtype=jnp.int32)
    all_codes = jnp.arange(depth_out * spread, dtype=jnp.int32)
    hits = (codes[:, None] == all_codes[None, :]) & (slots < count)[:, None]
    mask = jnp.any(hits, axis=0).astype(jnp.int32).reshape(depth_out, spread)
    filled = jnp.sum(mask, axis=1)
    pairs = (filled + 1) // 2
    index_out = jnp.arange(depth_out, dtype=jnp.int32)
    index_in = jnp.arange(spread, dtype=jnp.int32)
    base = jnp.sum(jnp.where(index_out[None, :] < index_out[:, None], pairs[None, :], 0), axis=1)
    rank = jnp.sum(
        jnp.where(index_in[None, None, :] < index_in[None, :, None], mask[:, None, :], 0), axis=2
    )
    place = jnp.where(mask > 0, 2 * base[:, None] + rank, -1).reshape(-1)
    spots = jnp.arange(2 * pairs_max, dtype=jnp.int32)
    found = jnp.sum(
        jnp.where(spots[:, None] == place[None, :], all_codes[None, :] + 1, 0), axis=1
    )
    found = found.reshape(pairs_max, 2)
    live = found > 0
    code = jnp.maximum(found - 1, 0)
    out_idx = jnp.where(live[:, 0], code[:, 0] // spread, depth_out - 1)
    in_idx = jnp.where(live, code % spread, spread)
    point = lookup(points, out_idx)
    return out_idx, in_idx[:, 0], in_idx[:, 1], point, jnp.sum(pairs).reshape(1)


def block_of(ref, block, blocks_dev, side):
    rows = pl.ds(pl.multiple_of(block % blocks_dev * side, side), side)
    return ref[block // blocks_dev, rows, :]


def add_pair(total_ref, fields_ref, tile, block, first, second):
    blocks_dev = fields_ref.shape[1] // total_ref.shape[1]
    side = total_ref.shape[1]
    both = jnp.concatenate(
        [block_of(fields_ref, place, blocks_dev, side) for place in (first, second)], axis=0
    )
    return total_ref, block, jnp.dot(tile, both, preferred_element_type=jnp.float32)


def build_kernel(
    blocks_dev,
    spread,
    slots_ref,
    out_ref_idx,
    first_idx,
    second_idx,
    point_idx,
    used_ref,
    coarse_a_ref,
    coarse_b_ref,
    over_in_ref,
    packed_a_ref,
    packed_i_ref,
    tiles_ref,
    total_ref,
    projected_ref,
    over_out_ref,
    fields_ref,
    sems,
):
    step = pl.program_id(0)
    side = total_ref.shape[1]
    depth = coarse_a_ref.shape[1]
    cols = packed_i_ref.shape[0]
    copies = (
        pltpu.make_async_copy(
            packed_a_ref.at[:, pl.ds(depth, blocks_dev * side), :], over_out_ref, sems.at[0]
        ),
        pltpu.make_async_copy(
            packed_i_ref.at[:, pl.ds(blocks_dev * depth, blocks_dev * side), :],
            fields_ref.at[pl.ds(0, cols)],
            sems.at[1],
        ),
    )

    @pl.when(step == 0)
    def _():
        for copy in copies:
            copy.start()
        total_ref[...] = jnp.zeros_like(total_ref)
        fields_ref[cols] = jnp.zeros(fields_ref.shape[1:], fields_ref.dtype)

    @pl.when(step < spread)
    def _():
        for a, ref in enumerate((coarse_a_ref, coarse_b_ref)):
            projected_ref[step * 2 + a] = jnp.dot(
                ref[0], over_in_ref[0], preferred_element_type=jnp.float32
            ).astype(jnp.bfloat16)

    @pl.when(step == spread)
    def _():
        for copy in copies:
            copy.wait()

    start = (step - spread) * chunk_pairs

    @pl.when((step >= spread) & (start < used_ref[0]))
    def _():
        def group(g, carry):
            adds = []
            for k in range(unroll_pairs):
                local = g * unroll_pairs + k
                pair = start + local
                block, first, second = out_ref_idx[pair], first_idx[pair], second_idx[pair]
                a = point_idx[pair]
                left = jnp.minimum(first, spread - 1) * 2 + a
                right = jnp.minimum(second, spread - 1) * 2 + a
                both = jnp.concatenate([projected_ref[left], projected_ref[right]], axis=1)
                tile = jnp.dot(
                    block_of(over_out_ref, block, blocks_dev, side),
                    both,
                    preferred_element_type=jnp.float32,
                ).astype(jnp.bfloat16)
                tiles_ref[local] = tile
                adds.append(add_pair(total_ref, fields_ref, tile, block, first, second))
            for ref, block, product in adds:
                ref[block] += product
            return carry

        lax.fori_loop(0, chunk_pairs // unroll_pairs, group, 0)


def apply_kernel_body(
    out_ref_idx,
    first_idx,
    second_idx,
    used_ref,
    tiles_ref,
    pieces_ref,
    total_ref,
    fields_ref,
):
    step = pl.program_id(0)
    cols = pieces_ref.shape[0]

    @pl.when(step == 0)
    def _():
        total_ref[...] = jnp.zeros_like(total_ref)
        fields_ref[pl.ds(0, cols)] = pieces_ref[...]
        fields_ref[cols] = jnp.zeros(fields_ref.shape[1:], fields_ref.dtype)

    start = step * chunk_pairs

    @pl.when(start < used_ref[0])
    def _():
        def group(g, carry):
            adds = []
            for k in range(chunk_pairs):
                local = g * chunk_pairs + k
                pair = start + local
                adds.append(
                    add_pair(
                        total_ref,
                        fields_ref,
                        tiles_ref[local],
                        out_ref_idx[pair],
                        first_idx[pair],
                        second_idx[pair],
                    )
                )
            for ref, block, product in adds:
                ref[block] += product
            return carry

        lax.fori_loop(0, chunk_pairs // chunk_pairs, group, 0)


def gather_kernel(a_ref, b_ref, i_ref, out_a, out_b, out_i, send_sem, recv_sem, own_sem):
    row, col = lax.axis_index("row"), lax.axis_index("col")
    h, z, k = row // 8, row // 2 % 4, row % 2
    l, x = col // 4, col % 4

    def row_of(hh, zz):
        return (hh * 4 + zz % 4) * 2 + k

    partner = (row_of(1 - h, z), col)
    z_dev = ((row_of(h, z + 1), col), (row_of(h, z + 3), col))
    x_dev = ((row, l * 4 + (x + 1) % 4), (row, l * 4 + (x + 3) % 4))
    sibling = (row + 1 - 2 * k, col)
    pair = (row, (1 - l) * 4 + x)

    barrier = pltpu.get_barrier_semaphore()
    neighbours = (partner, *z_dev, *x_dev, sibling, pair)
    for device in neighbours:
        pl.semaphore_signal(barrier, inc=1, device_id=device, device_id_type=MESH)
    pl.semaphore_wait(barrier, len(neighbours))

    def halves(ref):
        size = ref.shape[0] // 2
        return [pl.ds(s * size, size) for s in range(2)]

    half_a, half_b, half_i = halves(a_ref), halves(b_ref), halves(i_ref)
    copies, to_sibling = [], []

    def send(src, dst, device):
        copy = pltpu.make_async_remote_copy(
            src_ref=src,
            dst_ref=dst,
            send_sem=send_sem.at[len(copies)],
            recv_sem=recv_sem.at[len(copies)],
            device_id=device,
            device_id_type=MESH,
        )
        copy.start()
        copies.append(copy)
        return copy

    def pass_on(out, slot, part, device):
        return send(out.at[slot, part], out.at[slot, part], device)

    def share(out, slot):
        to_sibling.append(send(out.at[slot], out.at[slot], sibling))

    def forward(arrivals, out, slots, parts, devices):
        sent = []
        for d in range(2):
            arrivals[d][d].wait_recv()
            sent.append(pass_on(out, slots[d], parts[d], devices[d]))
        arrivals[0][1].wait_recv()
        arrivals[1][0].wait_recv()
        return sent

    a_y = [send(a_ref.at[p], out_a.at[row, p], partner) for p in half_a]
    b_z = [[send(b_ref.at[p], out_b.at[row, p], z_dev[d]) for p in half_b] for d in range(2)]
    i_x = [[send(i_ref.at[p], out_i.at[col, p], x_dev[d]) for p in half_i] for d in range(2)]
    to_sibling.append(send(a_ref, out_a.at[row], sibling))
    to_sibling.append(send(b_ref, out_b.at[row], sibling))
    own = [
        pltpu.make_async_copy(a_ref, out_a.at[row], own_sem.at[0]),
        pltpu.make_async_copy(b_ref, out_b.at[row], own_sem.at[1]),
        pltpu.make_async_copy(i_ref, out_i.at[col], own_sem.at[2]),
    ]
    for copy in own:
        copy.start()

    z_rows = (row_of(h, z + 3), row_of(h, z + 1))
    far = row_of(h, z + 2)
    x_cols = (l * 4 + (x + 3) % 4, l * 4 + (x + 1) % 4)
    other = row_of(1 - h, z)
    other_rows = (row_of(1 - h, z + 3), row_of(1 - h, z + 1))
    other_far = row_of(1 - h, z + 2)
    pair_col = (1 - l) * 4 + x
    other_cols = ((1 - l) * 4 + (x + 3) % 4, (1 - l) * 4 + (x + 1) % 4)

    b_zf = forward(b_z, out_b, z_rows, half_b, z_dev)
    a_z = [[send(a_ref.at[p], out_a.at[row, p], z_dev[d]) for p in half_a] for d in range(2)]
    for slot in z_rows:
        share(out_b, slot)
    a2_z = [[None, None], [None, None]]
    for s in range(2):
        a_y[s].wait_recv()
        for d in range(2):
            a2_z[d][s] = pass_on(out_a, other, half_a[s], z_dev[d])
    share(out_a, other)
    i_pair = send(i_ref, out_i.at[col], pair)
    b_y = [send(b_ref, out_b.at[row], partner)]
    for slot in z_rows:
        b_y.append(send(out_b.at[slot], out_b.at[slot], partner))
    i_xf = forward(i_x, out_i, x_cols, half_i, x_dev)
    for d in range(2):
        b_zf[d].wait_recv()
    b_y.append(send(out_b.at[far], out_b.at[far], partner))
    share(out_b, far)
    a_zf = forward(a_z, out_a, z_rows, half_a, z_dev)
    for slot in z_rows:
        share(out_a, slot)
    i_pair.wait_recv()
    i2_x = [[pass_on(out_i, pair_col, p, x_dev[d]) for p in half_i] for d in range(2)]
    for d in range(2):
        a_zf[d].wait_recv()
    share(out_a, far)
    i2_xf = forward(i2_x, out_i, other_cols, half_i, x_dev)
    a2_zf = forward(a2_z, out_a, other_rows, half_a, z_dev)
    for slot in other_rows:
        share(out_a, slot)
    for slot, copy in zip((other, *other_rows, other_far), b_y):
        copy.wait_recv()
        share(out_b, slot)
    for d in range(2):
        a2_zf[d].wait_recv()
    share(out_a, other_far)
    for copy in (*i_xf, *i2_xf, *to_sibling):
        copy.wait_recv()
    for copy in own:
        copy.wait()
    assert len(copies) == gather_copies
    for copy in copies:
        copy.wait_send()


def gather_all(a, b, i):
    rows, cols = lax.axis_size("row"), lax.axis_size("col")
    vmem = pl.BlockSpec(memory_space=pltpu.VMEM)
    anywhere = pl.BlockSpec(memory_space=pl.ANY)
    return pl.pallas_call(
        gather_kernel,
        in_specs=[vmem, vmem, vmem],
        out_specs=[anywhere] * 3,
        out_shape=[
            jax.ShapeDtypeStruct((rows, *a.shape), a.dtype),
            jax.ShapeDtypeStruct((rows, *b.shape), b.dtype),
            jax.ShapeDtypeStruct((cols, *i.shape), i.dtype),
        ],
        scratch_shapes=[
            pltpu.SemaphoreType.DMA((gather_copies,)),
            pltpu.SemaphoreType.DMA((gather_copies,)),
            pltpu.SemaphoreType.DMA((3,)),
        ],
        compiler_params=pltpu.CompilerParams(collective_id=0, has_side_effects=True),
        name="gather_all",
    )(a, b, i)


def exchange_kernel(spread_on, partial_ref, linear_ref, *refs):
    if spread_on:
        out_ref, pieces_ref, from_core, mine, landed, rounded, send_sem, recv_sem, own_sem = refs
    else:
        out_ref, from_core, mine, landed, send_sem, recv_sem = refs
    row, col = lax.axis_index("row"), lax.axis_index("col")
    h, z, k = row // 8, row // 2 % 4, row % 2
    l, x = col // 4, col % 4
    turns = ((1, 2), (1, 1), (1, 3), (0, 2), (1, 0), (0, 1), (0, 3), (0, 0))

    def row_of(turn, kk):
        return ((h + turn[0]) % 2 * 4 + (z + turn[1]) % 4) * 2 + kk

    def col_of(turn):
        return (l + turn[0]) % 2 * 4 + (x + turn[1]) % 4

    sibling = (row + 1 - 2 * k, col)
    neighbours = [sibling] + [(row_of(turn, k), col) for turn in turns[:-1]]
    if spread_on:
        neighbours += [(row, col_of(turn)) for turn in turns[:-1]]
    barrier = pltpu.get_barrier_semaphore()
    for device in neighbours:
        pl.semaphore_signal(barrier, inc=1, device_id=device, device_id_type=MESH)
    pl.semaphore_wait(barrier, len(neighbours))
    copies = []

    def send(src, dst, device):
        copy = pltpu.make_async_remote_copy(
            src_ref=src,
            dst_ref=dst,
            send_sem=send_sem.at[len(copies)],
            recv_sem=recv_sem.at[len(copies)],
            device_id=device,
            device_id_type=MESH,
        )
        copy.start()
        copies.append(copy)
        return copy

    peers = len(turns) - 1
    side = partial_ref.shape[1] // block_parts
    parts = [pl.ds(t * side, side) for t in range(block_parts)]
    crossed = [
        send(partial_ref.at[row_of(turn, 1 - k)], from_core.at[i], sibling)
        for i, turn in enumerate(turns)
    ]
    arrivals = []

    def send_on(i):
        device = (row_of(turns[i], k), col)
        arrivals.append([send(mine.at[i, p], landed.at[i, p], device) for p in parts])

    for i in range(peers):
        crossed[i].wait_recv()
        mine[i] = (partial_ref[row_of(turns[i], k)] + from_core[i]).astype(mine.dtype)
        if i > 0:
            send_on(i - 1)
    crossed[peers].wait_recv()
    send_on(peers - 1)
    spreads, own = [], []
    for t, p in enumerate(parts):
        total = partial_ref[row, p] + from_core[peers, p]
        for i in range(peers - 1, -1, -1):
            arrivals[i][t].wait_recv()
            total += landed[i, p].astype(jnp.float32)
        if spread_on:
            total = (linear_ref[p] + total) / spectrum_half
            rounded[p] = total.astype(rounded.dtype)
            out_ref[p] = total
            for turn in turns[:-1]:
                device = (row, col_of(turn))
                spreads.append(send(rounded.at[p], pieces_ref.at[col, p], device))
            own.append(pltpu.make_async_copy(rounded.at[p], pieces_ref.at[col, p], own_sem.at[t]))
            own[-1].start()
        else:
            out_ref[p] = total
    for copy in spreads:
        copy.wait_recv()
    for copy in own:
        copy.wait()
    for copy in copies:
        copy.wait_send()


def exchange(partial, linear, spread_on):
    rows, rows_dev, width = partial.shape
    cols = lax.axis_size("col")
    count = 8 + 7 * block_parts * (2 if spread_on else 1)
    vmem = pl.BlockSpec(memory_space=pltpu.VMEM)
    block = jax.ShapeDtypeStruct((rows_dev, width), jnp.float32)
    scratch = [
        pltpu.VMEM((8, rows_dev, width), jnp.float32),
        pltpu.VMEM((7, rows_dev, width), jnp.bfloat16),
        pltpu.VMEM((7, rows_dev, width), jnp.bfloat16),
    ]
    sems = [pltpu.SemaphoreType.DMA((count,)), pltpu.SemaphoreType.DMA((count,))]
    if spread_on:
        out_shape = [block, jax.ShapeDtypeStruct((cols, rows_dev, width), jnp.bfloat16)]
        out_specs = [vmem, pl.BlockSpec(memory_space=pl.ANY)]
        scratch.append(pltpu.VMEM((rows_dev, width), jnp.bfloat16))
        sems.append(pltpu.SemaphoreType.DMA((block_parts,)))
    else:
        out_shape, out_specs = block, vmem
    return pl.pallas_call(
        functools.partial(exchange_kernel, spread_on),
        in_specs=[vmem, vmem],
        out_specs=out_specs,
        out_shape=out_shape,
        scratch_shapes=scratch + sems,
        compiler_params=pltpu.CompilerParams(
            collective_id=1 if spread_on else 2, has_side_effects=True
        ),
        name="exchange_spread" if spread_on else "exchange",
    )(partial, linear)


def build_tiles(in_slots, tables, packed_a, packed_b, packed_i, pairs_max, blocks_dev, side):
    rows, cols = packed_a.shape[0], packed_i.shape[0]
    depth = packed_b.shape[1]
    width = packed_i.shape[2]
    spread, depth_out = cols * blocks_dev, rows * blocks_dev
    chunks = pairs_max // chunk_pairs

    def tile_chunk(s, *refs):
        last = jnp.maximum((refs[5][0] + chunk_pairs - 1) // chunk_pairs - 1, 0)
        return (jnp.clip(s - spread, 0, last), 0, 0)

    def coarse_at(s, slots, *refs):
        return (slots[jnp.minimum(s, spread - 1)], 0, 0)

    def over_in_at(s, *refs):
        block = jnp.minimum(s, spread - 1)
        return (block // blocks_dev, block % blocks_dev, 0)

    grid_spec = pltpu.PrefetchScalarGridSpec(
        num_scalar_prefetch=6,
        grid=(spread + chunks,),
        in_specs=[
            pl.BlockSpec((1, depth, depth), coarse_at),
            pl.BlockSpec((1, depth, depth), coarse_at),
            pl.BlockSpec((1, depth, side), over_in_at),
            pl.BlockSpec(memory_space=pl.ANY),
            pl.BlockSpec(memory_space=pl.ANY),
        ],
        out_specs=[
            pl.BlockSpec((chunk_pairs, side, 2 * side), tile_chunk),
            pl.BlockSpec((depth_out, side, width), lambda s, *refs: (0, 0, 0)),
        ],
        scratch_shapes=[
            pltpu.VMEM((spread * 2, depth, side), jnp.bfloat16),
            pltpu.VMEM((rows, blocks_dev * side, depth), jnp.bfloat16),
            pltpu.VMEM((cols + 1, blocks_dev * side, width), jnp.bfloat16),
            pltpu.SemaphoreType.DMA((2,)),
        ],
    )
    return pl.pallas_call(
        functools.partial(build_kernel, blocks_dev, spread),
        grid_spec=grid_spec,
        out_shape=[
            jax.ShapeDtypeStruct((pairs_max, side, 2 * side), jnp.bfloat16),
            jax.ShapeDtypeStruct((depth_out, side, width), jnp.float32),
        ],
        compiler_params=pltpu.CompilerParams(vmem_limit_bytes=60 * 1024 * 1024),
        name="build_tiles",
    )(in_slots, *tables, packed_a, packed_b, packed_i, packed_a, packed_i)


def apply_tiles(tables, tiles, pieces, depth_out):
    pairs_max, side, _ = tiles.shape
    cols, rows_dev, width = pieces.shape
    out_idx, first, second, _, used = tables

    def tile_chunk(s, *refs):
        last = jnp.maximum((refs[3][0] + chunk_pairs - 1) // chunk_pairs - 1, 0)
        return (jnp.minimum(s, last), 0, 0)

    def held(s, *refs):
        return (0, 0, 0)

    grid_spec = pltpu.PrefetchScalarGridSpec(
        num_scalar_prefetch=4,
        grid=(pairs_max // chunk_pairs,),
        in_specs=[
            pl.BlockSpec((chunk_pairs, side, 2 * side), tile_chunk),
            pl.BlockSpec(pieces.shape, held),
        ],
        out_specs=pl.BlockSpec((depth_out, side, width), held),
        scratch_shapes=[
            pltpu.VMEM((cols + 1, rows_dev, width), jnp.bfloat16),
        ],
    )
    return pl.pallas_call(
        apply_kernel_body,
        grid_spec=grid_spec,
        out_shape=jax.ShapeDtypeStruct((depth_out, side, width), jnp.float32),
        compiler_params=pltpu.CompilerParams(vmem_limit_bytes=60 * 1024 * 1024),
        name="apply_tiles",
    )(out_idx, first, second, used, tiles, pieces)


def on_device(
    vectors, energies, intersections, coarse, fine_coarse, coarse_slot, tile_codes, tile_count
):
    rows_count = lax.axis_size("row")
    cols_count = lax.axis_size("col")
    row_id = lax.axis_index("row")
    col_id = lax.axis_index("col")
    blocks_dev, pairs_coarse, tile_side = intersections.shape
    width_vec = vectors.shape[1]
    points_col = coarse.shape[0]
    spread = cols_count * blocks_dev
    depth_out = rows_count * blocks_dev
    pairs_max = (tile_codes.shape[1] + depth_out) // 2
    pairs_max = -(-pairs_max // chunk_pairs) * chunk_pairs
    index_out = jnp.arange(depth_out, dtype=jnp.int32)
    index_in = jnp.arange(spread, dtype=jnp.int32)
    out_blocks = (
        index_out // blocks_dev * cols_count + col_id
    ) * blocks_dev + index_out % blocks_dev
    in_blocks = (row_id * cols_count + index_in // blocks_dev) * blocks_dev + index_in % blocks_dev
    in_slots = lookup(coarse_slot, lookup(fine_coarse, in_blocks))
    out_points = lookup(fine_coarse, out_blocks) - col_id * points_col
    tables = pair_tables(
        tile_codes[0], tile_count[0], depth_out, spread, out_points, pairs_max
    )

    pair_energy = energies.reshape(-1, 1)
    across = jnp.swapaxes(intersections, 1, 2).reshape(-1, pairs_coarse)
    packed_a, packed_b, packed_i = gather_all(
        jnp.concatenate([coarse[0, 0], across], axis=0),
        coarse[1, 0],
        jnp.concatenate(
            [intersections.reshape(-1, tile_side), vectors.astype(jnp.bfloat16)], axis=0
        ),
    )

    def linear(field):
        return pair_energy * field - spectrum_center * field

    def by_row(partial):
        return partial.reshape(rows_count, -1, width_vec)

    tiles, partial = build_tiles(
        in_slots, tables, packed_a, packed_b, packed_i, pairs_max, blocks_dev, tile_side
    )
    first_step, pieces = exchange(by_row(partial), linear(vectors), True)
    partial = apply_tiles(tables, tiles, pieces, depth_out)
    kernel_part = exchange(by_row(partial), vectors, False)
    second_step = 2.0 * ((linear(first_step) + kernel_part) / spectrum_half) - vectors
    return first_step, second_step


def solution(mesh):
    in_specs = (
        P(("row", "col"), None),
        P(("row", "col")),
        P(("row", "col"), None, None),
        P("col", "row", None, None),
        P(),
        P(),
        P(("row", "col"), None),
        P(("row", "col")),
    )
    out_specs = (P(("row", "col"), None), P(("row", "col"), None))
    return jax.shard_map(
        on_device, mesh=mesh, in_specs=in_specs, out_specs=out_specs, check_vma=False
    )
```

```python
import functools

import jax
import jax.numpy as jnp
from jax import lax
from jax.experimental import pallas as pl
from jax.experimental.pallas import tpu as pltpu
from jax.sharding import PartitionSpec as P

spectrum_center = 2.0
spectrum_half = 3.0
unroll_blocks = 4
apply_group = 4
ring = 6
gather_copies = 53
block_parts = 3
MESH = pl.DeviceIdType.MESH


def lookup(values_table, positions):
    matches = positions[:, None] == jnp.arange(values_table.shape[0], dtype=jnp.int32)[None, :]
    return jnp.sum(jnp.where(matches, values_table[None, :], 0), axis=1)


def pair_tables(codes, count, depth_out, spread, points, pairs_max):
    slots = jnp.arange(codes.shape[0], dtype=jnp.int32)
    all_codes = jnp.arange(depth_out * spread, dtype=jnp.int32)
    hits = (codes[:, None] == all_codes[None, :]) & (slots < count)[:, None]
    mask = jnp.any(hits, axis=0).astype(jnp.int32).reshape(depth_out, spread)
    filled = jnp.sum(mask, axis=1)
    pairs = (filled + 1) // 2
    index_out = jnp.arange(depth_out, dtype=jnp.int32)
    index_in = jnp.arange(spread, dtype=jnp.int32)
    base = jnp.sum(jnp.where(index_out[None, :] < index_out[:, None], pairs[None, :], 0), axis=1)
    rank = jnp.sum(
        jnp.where(index_in[None, None, :] < index_in[None, :, None], mask[:, None, :], 0), axis=2
    )
    place = jnp.where(mask > 0, 2 * base[:, None] + rank, -1).reshape(-1)
    product = (index_in[None, :] * 2 + points[:, None]).reshape(-1)
    spots = jnp.arange(2 * pairs_max, dtype=jnp.int32)
    found = jnp.sum(jnp.where(spots[:, None] == place[None, :], product[None, :] + 1, 0), axis=1)
    return jnp.where(found > 0, found - 1, 2 * spread), base, pairs


def block_of(ref, block, blocks_dev, side):
    rows = pl.ds(pl.multiple_of(block % blocks_dev * side, side), side)
    return ref[block // blocks_dev, rows, :]


def sum_products(members_ref, base_ref, pairs_ref, products_ref, sums_ref, over_out_ref, out_ref):
    depth_out, side, width = out_ref.shape
    blocks_dev = over_out_ref.shape[1] // side
    depth = products_ref.shape[1]
    half = depth // 2

    def add_up(q, carry):
        start = base_ref[q]
        stop = start + pairs_ref[q]
        for c in range(2):
            rows = pl.ds(c * half, half)

            def add(pair, total):
                first, second = members_ref[2 * pair], members_ref[2 * pair + 1]
                return total + (products_ref[first, rows, :] + products_ref[second, rows, :])

            total = lax.fori_loop(start, stop, add, jnp.zeros((half, width), jnp.float32))
            sums_ref[q, rows, :] = total.astype(sums_ref.dtype)
        return carry

    lax.fori_loop(0, depth_out, add_up, 0)

    def finish(group, carry):
        for u in range(unroll_blocks):
            q = group * unroll_blocks + u
            out_ref[q] = jnp.dot(
                block_of(over_out_ref, q, blocks_dev, side),
                sums_ref[q],
                preferred_element_type=jnp.float32,
            )
        return carry

    lax.fori_loop(0, depth_out // unroll_blocks, finish, 0)


def build_kernel(
    blocks_dev,
    spread,
    slots_ref,
    members_ref,
    base_ref,
    pairs_ref,
    packed_a_ref,
    packed_b_ref,
    packed_i_ref,
    projected_ref,
    out_ref,
    products_ref,
    sums_ref,
    over_out_ref,
    sem,
    coarse_ref,
    over_in_ref,
    field_ref,
    ring_sems,
):
    step = pl.program_id(0)
    side = out_ref.shape[1]
    depth = packed_b_ref.shape[1]

    def reads(block, place):
        slot = slots_ref[block]
        owner, local = block // blocks_dev, block % blocks_dev
        over_rows = pl.ds(pl.multiple_of(local * depth, depth), depth)
        field_rows = pl.ds(pl.multiple_of(blocks_dev * depth + local * side, side), side)
        sources = (
            (packed_a_ref.at[slot, pl.ds(0, depth), :], coarse_ref.at[place, 0]),
            (packed_b_ref.at[slot], coarse_ref.at[place, 1]),
            (packed_i_ref.at[owner, over_rows, :], over_in_ref.at[place]),
            (packed_i_ref.at[owner, field_rows, :], field_ref.at[place]),
        )
        return [
            pltpu.make_async_copy(src, dst, ring_sems.at[place, n])
            for n, (src, dst) in enumerate(sources)
        ]

    copy = pltpu.make_async_copy(
        packed_a_ref.at[:, pl.ds(depth, blocks_dev * side), :], over_out_ref, sem
    )

    @pl.when(step == 0)
    def _():
        for block in range(ring):
            for read in reads(block, block):
                read.start()
        copy.start()
        products_ref[2 * spread] = jnp.zeros(products_ref.shape[1:], products_ref.dtype)

    place = step % ring
    for read in reads(step, place):
        read.wait()
    for a in range(2):
        projected = jnp.dot(
            coarse_ref[place, a], over_in_ref[place], preferred_element_type=jnp.float32
        ).astype(jnp.bfloat16)
        projected_ref[a] = projected
        products_ref[step * 2 + a] = jnp.dot(
            projected, field_ref[place], preferred_element_type=jnp.float32
        )

    @pl.when(step + ring < spread)
    def _():
        for read in reads(step + ring, place):
            read.start()

    @pl.when(step == pl.num_programs(0) - 1)
    def _():
        copy.wait()
        sum_products(
            members_ref, base_ref, pairs_ref, products_ref, sums_ref, over_out_ref, out_ref
        )


def apply_kernel_body(
    blocks_dev,
    spread,
    members_ref,
    base_ref,
    pairs_ref,
    projected_ref,
    pieces_ref,
    packed_a_ref,
    out_ref,
    products_ref,
    sums_ref,
    over_out_ref,
    sem,
    held_ref,
    group_sems,
):
    step = pl.program_id(0)
    side = out_ref.shape[1]
    depth = projected_ref.shape[1]
    groups = spread // apply_group
    reads = [
        pltpu.make_async_copy(
            projected_ref.at[pl.ds(2 * apply_group * g, 2 * apply_group)],
            held_ref.at[pl.ds(2 * apply_group * g, 2 * apply_group)],
            group_sems.at[g],
        )
        for g in range(groups)
    ]
    copy = pltpu.make_async_copy(
        packed_a_ref.at[:, pl.ds(depth, blocks_dev * side), :], over_out_ref, sem
    )

    @pl.when(step == 0)
    def _():
        for read in reads:
            read.start()
        copy.start()
        products_ref[2 * spread] = jnp.zeros(products_ref.shape[1:], products_ref.dtype)

    for g, read in enumerate(reads):
        pl.when(step == g)(read.wait)

    for g in range(apply_group):
        block = step * apply_group + g
        field = block_of(pieces_ref, block, blocks_dev, side)
        for a in range(2):
            products_ref[block * 2 + a] = jnp.dot(
                held_ref[block * 2 + a], field, preferred_element_type=jnp.float32
            )

    @pl.when(step == pl.num_programs(0) - 1)
    def _():
        copy.wait()
        sum_products(
            members_ref, base_ref, pairs_ref, products_ref, sums_ref, over_out_ref, out_ref
        )


def gather_kernel(a_ref, b_ref, i_ref, out_a, out_b, out_i, send_sem, recv_sem, own_sem):
    row, col = lax.axis_index("row"), lax.axis_index("col")
    h, z, k = row // 8, row // 2 % 4, row % 2
    l, x = col // 4, col % 4

    def row_of(hh, zz):
        return (hh * 4 + zz % 4) * 2 + k

    partner = (row_of(1 - h, z), col)
    z_dev = ((row_of(h, z + 1), col), (row_of(h, z + 3), col))
    x_dev = ((row, l * 4 + (x + 1) % 4), (row, l * 4 + (x + 3) % 4))
    sibling = (row + 1 - 2 * k, col)
    pair = (row, (1 - l) * 4 + x)

    barrier = pltpu.get_barrier_semaphore()
    neighbours = (partner, *z_dev, *x_dev, sibling, pair)
    for device in neighbours:
        pl.semaphore_signal(barrier, inc=1, device_id=device, device_id_type=MESH)
    pl.semaphore_wait(barrier, len(neighbours))

    def halves(ref):
        size = ref.shape[0] // 2
        return [pl.ds(s * size, size) for s in range(2)]

    half_a, half_b, half_i = halves(a_ref), halves(b_ref), halves(i_ref)
    copies, to_sibling = [], []

    def send(src, dst, device):
        copy = pltpu.make_async_remote_copy(
            src_ref=src,
            dst_ref=dst,
            send_sem=send_sem.at[len(copies)],
            recv_sem=recv_sem.at[len(copies)],
            device_id=device,
            device_id_type=MESH,
        )
        copy.start()
        copies.append(copy)
        return copy

    def pass_on(out, slot, part, device):
        return send(out.at[slot, part], out.at[slot, part], device)

    def share(out, slot):
        to_sibling.append(send(out.at[slot], out.at[slot], sibling))

    def forward(arrivals, out, slots, parts, devices):
        sent = []
        for d in range(2):
            arrivals[d][d].wait_recv()
            sent.append(pass_on(out, slots[d], parts[d], devices[d]))
        arrivals[0][1].wait_recv()
        arrivals[1][0].wait_recv()
        return sent

    a_y = [send(a_ref.at[p], out_a.at[row, p], partner) for p in half_a]
    b_z = [[send(b_ref.at[p], out_b.at[row, p], z_dev[d]) for p in half_b] for d in range(2)]
    i_x = [[send(i_ref.at[p], out_i.at[col, p], x_dev[d]) for p in half_i] for d in range(2)]
    to_sibling.append(send(a_ref, out_a.at[row], sibling))
    to_sibling.append(send(b_ref, out_b.at[row], sibling))
    own = [
        pltpu.make_async_copy(a_ref, out_a.at[row], own_sem.at[0]),
        pltpu.make_async_copy(b_ref, out_b.at[row], own_sem.at[1]),
        pltpu.make_async_copy(i_ref, out_i.at[col], own_sem.at[2]),
    ]
    for copy in own:
        copy.start()

    z_rows = (row_of(h, z + 3), row_of(h, z + 1))
    far = row_of(h, z + 2)
    x_cols = (l * 4 + (x + 3) % 4, l * 4 + (x + 1) % 4)
    other = row_of(1 - h, z)
    other_rows = (row_of(1 - h, z + 3), row_of(1 - h, z + 1))
    other_far = row_of(1 - h, z + 2)
    pair_col = (1 - l) * 4 + x
    other_cols = ((1 - l) * 4 + (x + 3) % 4, (1 - l) * 4 + (x + 1) % 4)

    b_zf = forward(b_z, out_b, z_rows, half_b, z_dev)
    a_z = [[send(a_ref.at[p], out_a.at[row, p], z_dev[d]) for p in half_a] for d in range(2)]
    for slot in z_rows:
        share(out_b, slot)
    a2_z = [[None, None], [None, None]]
    for s in range(2):
        a_y[s].wait_recv()
        for d in range(2):
            a2_z[d][s] = pass_on(out_a, other, half_a[s], z_dev[d])
    share(out_a, other)
    i_pair = send(i_ref, out_i.at[col], pair)
    b_y = [send(b_ref, out_b.at[row], partner)]
    for slot in z_rows:
        b_y.append(send(out_b.at[slot], out_b.at[slot], partner))
    i_xf = forward(i_x, out_i, x_cols, half_i, x_dev)
    for d in range(2):
        b_zf[d].wait_recv()
    b_y.append(send(out_b.at[far], out_b.at[far], partner))
    share(out_b, far)
    a_zf = forward(a_z, out_a, z_rows, half_a, z_dev)
    for slot in z_rows:
        share(out_a, slot)
    i_pair.wait_recv()
    i2_x = [[pass_on(out_i, pair_col, p, x_dev[d]) for p in half_i] for d in range(2)]
    for d in range(2):
        a_zf[d].wait_recv()
    share(out_a, far)
    i2_xf = forward(i2_x, out_i, other_cols, half_i, x_dev)
    a2_zf = forward(a2_z, out_a, other_rows, half_a, z_dev)
    for slot in other_rows:
        share(out_a, slot)
    for slot, copy in zip((other, *other_rows, other_far), b_y):
        copy.wait_recv()
        share(out_b, slot)
    for d in range(2):
        a2_zf[d].wait_recv()
    share(out_a, other_far)
    for copy in (*i_xf, *i2_xf, *to_sibling):
        copy.wait_recv()
    for copy in own:
        copy.wait()
    assert len(copies) == gather_copies
    for copy in copies:
        copy.wait_send()


def gather_all(a, b, i):
    rows, cols = lax.axis_size("row"), lax.axis_size("col")
    vmem = pl.BlockSpec(memory_space=pltpu.VMEM)
    anywhere = pl.BlockSpec(memory_space=pl.ANY)
    return pl.pallas_call(
        gather_kernel,
        in_specs=[vmem, vmem, vmem],
        out_specs=[anywhere] * 3,
        out_shape=[
            jax.ShapeDtypeStruct((rows, *a.shape), a.dtype),
            jax.ShapeDtypeStruct((rows, *b.shape), b.dtype),
            jax.ShapeDtypeStruct((cols, *i.shape), i.dtype),
        ],
        scratch_shapes=[
            pltpu.SemaphoreType.DMA((gather_copies,)),
            pltpu.SemaphoreType.DMA((gather_copies,)),
            pltpu.SemaphoreType.DMA((3,)),
        ],
        compiler_params=pltpu.CompilerParams(collective_id=0, has_side_effects=True),
        name="gather_all",
    )(a, b, i)


def exchange_kernel(spread_on, partial_ref, linear_ref, *refs):
    if spread_on:
        out_ref, pieces_ref, from_core, mine, landed, rounded, send_sem, recv_sem, own_sem = refs
    else:
        out_ref, from_core, mine, landed, send_sem, recv_sem = refs
    row, col = lax.axis_index("row"), lax.axis_index("col")
    h, z, k = row // 8, row // 2 % 4, row % 2
    l, x = col // 4, col % 4
    turns = ((1, 2), (1, 1), (1, 3), (0, 2), (1, 0), (0, 1), (0, 3), (0, 0))

    def row_of(turn, kk):
        return ((h + turn[0]) % 2 * 4 + (z + turn[1]) % 4) * 2 + kk

    def col_of(turn):
        return (l + turn[0]) % 2 * 4 + (x + turn[1]) % 4

    sibling = (row + 1 - 2 * k, col)
    neighbours = [sibling] + [(row_of(turn, k), col) for turn in turns[:-1]]
    if spread_on:
        neighbours += [(row, col_of(turn)) for turn in turns[:-1]]
    barrier = pltpu.get_barrier_semaphore()
    for device in neighbours:
        pl.semaphore_signal(barrier, inc=1, device_id=device, device_id_type=MESH)
    pl.semaphore_wait(barrier, len(neighbours))
    copies = []

    def send(src, dst, device):
        copy = pltpu.make_async_remote_copy(
            src_ref=src,
            dst_ref=dst,
            send_sem=send_sem.at[len(copies)],
            recv_sem=recv_sem.at[len(copies)],
            device_id=device,
            device_id_type=MESH,
        )
        copy.start()
        copies.append(copy)
        return copy

    peers = len(turns) - 1
    side = partial_ref.shape[1] // block_parts
    parts = [pl.ds(t * side, side) for t in range(block_parts)]
    crossed = [
        send(partial_ref.at[row_of(turn, 1 - k)], from_core.at[i], sibling)
        for i, turn in enumerate(turns)
    ]
    arrivals = []

    def send_on(i):
        device = (row_of(turns[i], k), col)
        arrivals.append([send(mine.at[i, p], landed.at[i, p], device) for p in parts])

    for i in range(peers):
        crossed[i].wait_recv()
        mine[i] = (partial_ref[row_of(turns[i], k)] + from_core[i]).astype(mine.dtype)
        if i > 0:
            send_on(i - 1)
    crossed[peers].wait_recv()
    send_on(peers - 1)
    spreads, own = [], []
    for t, p in enumerate(parts):
        total = partial_ref[row, p] + from_core[peers, p]
        for i in range(peers - 1, -1, -1):
            arrivals[i][t].wait_recv()
            total += landed[i, p].astype(jnp.float32)
        if spread_on:
            total = (linear_ref[p] + total) / spectrum_half
            rounded[p] = total.astype(rounded.dtype)
            out_ref[p] = total
            for turn in turns[:-1]:
                device = (row, col_of(turn))
                spreads.append(send(rounded.at[p], pieces_ref.at[col, p], device))
            own.append(pltpu.make_async_copy(rounded.at[p], pieces_ref.at[col, p], own_sem.at[t]))
            own[-1].start()
        else:
            out_ref[p] = total
    for copy in spreads:
        copy.wait_recv()
    for copy in own:
        copy.wait()
    for copy in copies:
        copy.wait_send()


def exchange(partial, linear, spread_on):
    rows, rows_dev, width = partial.shape
    cols = lax.axis_size("col")
    count = 8 + 7 * block_parts * (2 if spread_on else 1)
    vmem = pl.BlockSpec(memory_space=pltpu.VMEM)
    block = jax.ShapeDtypeStruct((rows_dev, width), jnp.float32)
    scratch = [
        pltpu.VMEM((8, rows_dev, width), jnp.float32),
        pltpu.VMEM((7, rows_dev, width), jnp.bfloat16),
        pltpu.VMEM((7, rows_dev, width), jnp.bfloat16),
    ]
    sems = [pltpu.SemaphoreType.DMA((count,)), pltpu.SemaphoreType.DMA((count,))]
    if spread_on:
        out_shape = [block, jax.ShapeDtypeStruct((cols, rows_dev, width), jnp.bfloat16)]
        out_specs = [vmem, pl.BlockSpec(memory_space=pl.ANY)]
        scratch.append(pltpu.VMEM((rows_dev, width), jnp.bfloat16))
        sems.append(pltpu.SemaphoreType.DMA((block_parts,)))
    else:
        out_shape, out_specs = block, vmem
    return pl.pallas_call(
        functools.partial(exchange_kernel, spread_on),
        in_specs=[vmem, vmem],
        out_specs=out_specs,
        out_shape=out_shape,
        scratch_shapes=scratch + sems,
        compiler_params=pltpu.CompilerParams(
            collective_id=1 if spread_on else 2, has_side_effects=True
        ),
        name="exchange_spread" if spread_on else "exchange",
    )(partial, linear)


def apply_scratch(rows, blocks_dev, spread, depth, side, width):
    return [
        pltpu.VMEM((2 * spread + 1, depth, width), jnp.float32),
        pltpu.VMEM((rows * blocks_dev, depth, width), jnp.bfloat16),
        pltpu.VMEM((rows, blocks_dev * side, depth), jnp.bfloat16),
        pltpu.SemaphoreType.DMA,
    ]


def project_and_apply(in_slots, tables, packed_a, packed_b, packed_i, blocks_dev, side):
    rows, cols = packed_a.shape[0], packed_i.shape[0]
    depth = packed_b.shape[1]
    width = packed_i.shape[2]
    spread, depth_out = cols * blocks_dev, rows * blocks_dev
    anywhere = pl.BlockSpec(memory_space=pl.ANY)
    grid_spec = pltpu.PrefetchScalarGridSpec(
        num_scalar_prefetch=4,
        grid=(spread,),
        in_specs=[anywhere] * 3,
        out_specs=[
            pl.BlockSpec((2, depth, side), lambda s, *refs: (s, 0, 0)),
            pl.BlockSpec((depth_out, side, width), lambda s, *refs: (0, 0, 0)),
        ],
        scratch_shapes=[
            *apply_scratch(rows, blocks_dev, spread, depth, side, width),
            pltpu.VMEM((ring, 2, depth, depth), jnp.bfloat16),
            pltpu.VMEM((ring, depth, side), jnp.bfloat16),
            pltpu.VMEM((ring, side, width), jnp.bfloat16),
            pltpu.SemaphoreType.DMA((ring, 4)),
        ],
    )
    return pl.pallas_call(
        functools.partial(build_kernel, blocks_dev, spread),
        grid_spec=grid_spec,
        out_shape=[
            jax.ShapeDtypeStruct((2 * spread, depth, side), jnp.bfloat16),
            jax.ShapeDtypeStruct((depth_out, side, width), jnp.float32),
        ],
        compiler_params=pltpu.CompilerParams(vmem_limit_bytes=60 * 1024 * 1024),
        name="project_and_apply",
    )(in_slots, *tables, packed_a, packed_b, packed_i)


def apply_again(tables, projected, pieces, packed_a, blocks_dev):
    rows = packed_a.shape[0]
    _, depth, side = projected.shape
    cols, _, width = pieces.shape
    spread, depth_out = cols * blocks_dev, rows * blocks_dev
    grid_spec = pltpu.PrefetchScalarGridSpec(
        num_scalar_prefetch=3,
        grid=(spread // apply_group,),
        in_specs=[
            pl.BlockSpec(memory_space=pl.ANY),
            pl.BlockSpec(pieces.shape, lambda s, *refs: (0, 0, 0)),
            pl.BlockSpec(memory_space=pl.ANY),
        ],
        out_specs=pl.BlockSpec((depth_out, side, width), lambda s, *refs: (0, 0, 0)),
        scratch_shapes=[
            *apply_scratch(rows, blocks_dev, spread, depth, side, width),
            pltpu.VMEM(projected.shape, jnp.bfloat16),
            pltpu.SemaphoreType.DMA((spread // apply_group,)),
        ],
    )
    return pl.pallas_call(
        functools.partial(apply_kernel_body, blocks_dev, spread),
        grid_spec=grid_spec,
        out_shape=jax.ShapeDtypeStruct((depth_out, side, width), jnp.float32),
        compiler_params=pltpu.CompilerParams(vmem_limit_bytes=60 * 1024 * 1024),
        name="apply_again",
    )(*tables, projected, pieces, packed_a)


def on_device(
    vectors, energies, intersections, coarse, fine_coarse, coarse_slot, tile_codes, tile_count
):
    rows_count = lax.axis_size("row")
    cols_count = lax.axis_size("col")
    row_id = lax.axis_index("row")
    col_id = lax.axis_index("col")
    blocks_dev, pairs_coarse, tile_side = intersections.shape
    width_vec = vectors.shape[1]
    points_col = coarse.shape[0]
    spread = cols_count * blocks_dev
    depth_out = rows_count * blocks_dev
    pairs_max = (tile_codes.shape[1] + depth_out) // 2
    index_out = jnp.arange(depth_out, dtype=jnp.int32)
    index_in = jnp.arange(spread, dtype=jnp.int32)
    out_blocks = (
        index_out // blocks_dev * cols_count + col_id
    ) * blocks_dev + index_out % blocks_dev
    in_blocks = (row_id * cols_count + index_in // blocks_dev) * blocks_dev + index_in % blocks_dev
    in_slots = lookup(coarse_slot, lookup(fine_coarse, in_blocks))
    out_points = lookup(fine_coarse, out_blocks) - col_id * points_col
    tables = pair_tables(
        tile_codes[0], tile_count[0], depth_out, spread, out_points, pairs_max
    )

    pair_energy = energies.reshape(-1, 1)
    across = jnp.swapaxes(intersections, 1, 2).reshape(-1, pairs_coarse)
    packed_a, packed_b, packed_i = gather_all(
        jnp.concatenate([coarse[0, 0], across], axis=0),
        coarse[1, 0],
        jnp.concatenate(
            [intersections.reshape(-1, tile_side), vectors.astype(jnp.bfloat16)], axis=0
        ),
    )

    def linear(field):
        return pair_energy * field - spectrum_center * field

    def by_row(partial):
        return partial.reshape(rows_count, -1, width_vec)

    projected, partial = project_and_apply(
        in_slots, tables, packed_a, packed_b, packed_i, blocks_dev, tile_side
    )
    first_step, pieces = exchange(by_row(partial), linear(vectors), True)
    partial = apply_again(tables, projected, pieces, packed_a, blocks_dev)
    kernel_part = exchange(by_row(partial), vectors, False)
    second_step = 2.0 * ((linear(first_step) + kernel_part) / spectrum_half) - vectors
    return first_step, second_step


def solution(mesh):
    in_specs = (
        P(("row", "col"), None),
        P(("row", "col")),
        P(("row", "col"), None, None),
        P("col", "row", None, None),
        P(),
        P(),
        P(("row", "col"), None),
        P(("row", "col")),
    )
    out_specs = (P(("row", "col"), None), P(("row", "col"), None))
    return jax.shard_map(
        on_device, mesh=mesh, in_specs=in_specs, out_specs=out_specs, check_vma=False
    )
```

```python
import functools

import jax
import jax.numpy as jnp
from jax import lax
from jax.experimental import pallas as pl
from jax.experimental.pallas import tpu as pltpu
from jax.sharding import PartitionSpec as P

spectrum_center = 2.0
spectrum_half = 3.0
unroll_blocks = 4
apply_group = 4
list_group = 4
sum_rows = 128
ring = 6
gather_copies = 53
block_parts = 3
MESH = pl.DeviceIdType.MESH


def lookup(values_table, positions):
    matches = positions[:, None] == jnp.arange(values_table.shape[0], dtype=jnp.int32)[None, :]
    return jnp.sum(jnp.where(matches, values_table[None, :], 0), axis=1)


def list_tables(codes, count, depth_out, spread, points, groups_max):
    slots = jnp.arange(codes.shape[0], dtype=jnp.int32)
    all_codes = jnp.arange(depth_out * spread, dtype=jnp.int32)
    hits = (codes[:, None] == all_codes[None, :]) & (slots < count)[:, None]
    mask = jnp.any(hits, axis=0).astype(jnp.int32).reshape(depth_out, spread)
    filled = jnp.sum(mask, axis=1)
    groups = (filled + list_group - 1) // list_group
    index_out = jnp.arange(depth_out, dtype=jnp.int32)
    index_in = jnp.arange(spread, dtype=jnp.int32)
    base = jnp.sum(jnp.where(index_out[None, :] < index_out[:, None], groups[None, :], 0), axis=1)
    rank = jnp.sum(
        jnp.where(index_in[None, None, :] < index_in[None, :, None], mask[:, None, :], 0), axis=2
    )
    place = jnp.where(mask > 0, list_group * base[:, None] + rank, -1).reshape(-1)
    product = (index_in[None, :] * 2 + points[:, None]).reshape(-1)
    spots = jnp.arange(list_group * groups_max, dtype=jnp.int32)
    found = jnp.sum(jnp.where(spots[:, None] == place[None, :], product[None, :] + 1, 0), axis=1)
    return jnp.where(found > 0, found - 1, 2 * spread), base, groups


def block_of(ref, block, blocks_dev, side):
    rows = pl.ds(pl.multiple_of(block % blocks_dev * side, side), side)
    return ref[block // blocks_dev, rows, :]


def sum_products(members_ref, base_ref, groups_ref, products_ref, sums_ref, over_out_ref, out_ref):
    depth_out, side, width = out_ref.shape
    blocks_dev = over_out_ref.shape[1] // side
    depth = products_ref.shape[1]

    def add_up(q, carry):
        start = base_ref[q]
        stop = start + groups_ref[q]
        for c in range(depth // sum_rows):
            rows = pl.ds(c * sum_rows, sum_rows)

            def add(group, total):
                parts = [
                    products_ref[members_ref[list_group * group + n], rows, :]
                    for n in range(list_group)
                ]
                while len(parts) > 1:
                    parts = [left + right for left, right in zip(parts[::2], parts[1::2])]
                return total + parts[0]

            total = lax.fori_loop(start, stop, add, jnp.zeros((sum_rows, width), jnp.float32))
            sums_ref[q, rows, :] = total.astype(sums_ref.dtype)
        return carry

    lax.fori_loop(0, depth_out, add_up, 0)

    def finish(group, carry):
        for u in range(unroll_blocks):
            q = group * unroll_blocks + u
            out_ref[q] = jnp.dot(
                block_of(over_out_ref, q, blocks_dev, side),
                sums_ref[q],
                preferred_element_type=jnp.float32,
            )
        return carry

    lax.fori_loop(0, depth_out // unroll_blocks, finish, 0)


def build_kernel(
    blocks_dev,
    spread,
    slots_ref,
    members_ref,
    base_ref,
    groups_ref,
    packed_a_ref,
    packed_b_ref,
    packed_i_ref,
    projected_ref,
    out_ref,
    products_ref,
    sums_ref,
    over_out_ref,
    sem,
    coarse_ref,
    over_in_ref,
    field_ref,
    ring_sems,
):
    step = pl.program_id(0)
    side = out_ref.shape[1]
    depth = packed_b_ref.shape[1]

    def reads(block, place):
        slot = slots_ref[block]
        owner, local = block // blocks_dev, block % blocks_dev
        over_rows = pl.ds(pl.multiple_of(local * depth, depth), depth)
        field_rows = pl.ds(pl.multiple_of(blocks_dev * depth + local * side, side), side)
        sources = (
            (packed_a_ref.at[slot, pl.ds(0, depth), :], coarse_ref.at[place, 0]),
            (packed_b_ref.at[slot], coarse_ref.at[place, 1]),
            (packed_i_ref.at[owner, over_rows, :], over_in_ref.at[place]),
            (packed_i_ref.at[owner, field_rows, :], field_ref.at[place]),
        )
        return [
            pltpu.make_async_copy(src, dst, ring_sems.at[place, n])
            for n, (src, dst) in enumerate(sources)
        ]

    copy = pltpu.make_async_copy(
        packed_a_ref.at[:, pl.ds(depth, blocks_dev * side), :], over_out_ref, sem
    )

    @pl.when(step == 0)
    def _():
        for block in range(ring):
            for read in reads(block, block):
                read.start()
        copy.start()
        products_ref[2 * spread] = jnp.zeros(products_ref.shape[1:], products_ref.dtype)

    place = step % ring
    for read in reads(step, place):
        read.wait()
    for a in range(2):
        projected = jnp.dot(
            coarse_ref[place, a], over_in_ref[place], preferred_element_type=jnp.float32
        ).astype(jnp.bfloat16)
        projected_ref[a] = projected
        products_ref[step * 2 + a] = jnp.dot(
            projected, field_ref[place], preferred_element_type=jnp.float32
        )

    @pl.when(step + ring < spread)
    def _():
        for read in reads(step + ring, place):
            read.start()

    @pl.when(step == pl.num_programs(0) - 1)
    def _():
        copy.wait()
        sum_products(
            members_ref, base_ref, groups_ref, products_ref, sums_ref, over_out_ref, out_ref
        )


def apply_kernel_body(
    blocks_dev,
    spread,
    members_ref,
    base_ref,
    groups_ref,
    projected_ref,
    pieces_ref,
    packed_a_ref,
    out_ref,
    products_ref,
    sums_ref,
    over_out_ref,
    sem,
    held_ref,
    group_sems,
):
    step = pl.program_id(0)
    side = out_ref.shape[1]
    depth = projected_ref.shape[1]
    groups = spread // apply_group
    reads = [
        pltpu.make_async_copy(
            projected_ref.at[pl.ds(2 * apply_group * g, 2 * apply_group)],
            held_ref.at[pl.ds(2 * apply_group * g, 2 * apply_group)],
            group_sems.at[g],
        )
        for g in range(groups)
    ]
    copy = pltpu.make_async_copy(
        packed_a_ref.at[:, pl.ds(depth, blocks_dev * side), :], over_out_ref, sem
    )

    @pl.when(step == 0)
    def _():
        for read in reads:
            read.start()
        copy.start()
        products_ref[2 * spread] = jnp.zeros(products_ref.shape[1:], products_ref.dtype)

    for g, read in enumerate(reads):
        pl.when(step == g)(read.wait)

    for g in range(apply_group):
        block = step * apply_group + g
        field = block_of(pieces_ref, block, blocks_dev, side)
        for a in range(2):
            products_ref[block * 2 + a] = jnp.dot(
                held_ref[block * 2 + a], field, preferred_element_type=jnp.float32
            )

    @pl.when(step == pl.num_programs(0) - 1)
    def _():
        copy.wait()
        sum_products(
            members_ref, base_ref, groups_ref, products_ref, sums_ref, over_out_ref, out_ref
        )


def gather_kernel(a_ref, b_ref, i_ref, out_a, out_b, out_i, send_sem, recv_sem, own_sem):
    row, col = lax.axis_index("row"), lax.axis_index("col")
    h, z, k = row // 8, row // 2 % 4, row % 2
    l, x = col // 4, col % 4

    def row_of(hh, zz):
        return (hh * 4 + zz % 4) * 2 + k

    partner = (row_of(1 - h, z), col)
    z_dev = ((row_of(h, z + 1), col), (row_of(h, z + 3), col))
    x_dev = ((row, l * 4 + (x + 1) % 4), (row, l * 4 + (x + 3) % 4))
    sibling = (row + 1 - 2 * k, col)
    pair = (row, (1 - l) * 4 + x)

    barrier = pltpu.get_barrier_semaphore()
    neighbours = (partner, *z_dev, *x_dev, sibling, pair)
    for device in neighbours:
        pl.semaphore_signal(barrier, inc=1, device_id=device, device_id_type=MESH)
    pl.semaphore_wait(barrier, len(neighbours))

    def halves(ref):
        size = ref.shape[0] // 2
        return [pl.ds(s * size, size) for s in range(2)]

    half_a, half_b, half_i = halves(a_ref), halves(b_ref), halves(i_ref)
    copies, to_sibling = [], []

    def send(src, dst, device):
        copy = pltpu.make_async_remote_copy(
            src_ref=src,
            dst_ref=dst,
            send_sem=send_sem.at[len(copies)],
            recv_sem=recv_sem.at[len(copies)],
            device_id=device,
            device_id_type=MESH,
        )
        copy.start()
        copies.append(copy)
        return copy

    def pass_on(out, slot, part, device):
        return send(out.at[slot, part], out.at[slot, part], device)

    def share(out, slot):
        to_sibling.append(send(out.at[slot], out.at[slot], sibling))

    def forward(arrivals, out, slots, parts, devices):
        sent = []
        for d in range(2):
            arrivals[d][d].wait_recv()
            sent.append(pass_on(out, slots[d], parts[d], devices[d]))
        arrivals[0][1].wait_recv()
        arrivals[1][0].wait_recv()
        return sent

    a_y = [send(a_ref.at[p], out_a.at[row, p], partner) for p in half_a]
    b_z = [[send(b_ref.at[p], out_b.at[row, p], z_dev[d]) for p in half_b] for d in range(2)]
    i_x = [[send(i_ref.at[p], out_i.at[col, p], x_dev[d]) for p in half_i] for d in range(2)]
    to_sibling.append(send(a_ref, out_a.at[row], sibling))
    to_sibling.append(send(b_ref, out_b.at[row], sibling))
    own = [
        pltpu.make_async_copy(a_ref, out_a.at[row], own_sem.at[0]),
        pltpu.make_async_copy(b_ref, out_b.at[row], own_sem.at[1]),
        pltpu.make_async_copy(i_ref, out_i.at[col], own_sem.at[2]),
    ]
    for copy in own:
        copy.start()

    z_rows = (row_of(h, z + 3), row_of(h, z + 1))
    far = row_of(h, z + 2)
    x_cols = (l * 4 + (x + 3) % 4, l * 4 + (x + 1) % 4)
    other = row_of(1 - h, z)
    other_rows = (row_of(1 - h, z + 3), row_of(1 - h, z + 1))
    other_far = row_of(1 - h, z + 2)
    pair_col = (1 - l) * 4 + x
    other_cols = ((1 - l) * 4 + (x + 3) % 4, (1 - l) * 4 + (x + 1) % 4)

    b_zf = forward(b_z, out_b, z_rows, half_b, z_dev)
    a_z = [[send(a_ref.at[p], out_a.at[row, p], z_dev[d]) for p in half_a] for d in range(2)]
    for slot in z_rows:
        share(out_b, slot)
    a2_z = [[None, None], [None, None]]
    for s in range(2):
        a_y[s].wait_recv()
        for d in range(2):
            a2_z[d][s] = pass_on(out_a, other, half_a[s], z_dev[d])
    share(out_a, other)
    i_pair = send(i_ref, out_i.at[col], pair)
    b_y = [send(b_ref, out_b.at[row], partner)]
    for slot in z_rows:
        b_y.append(send(out_b.at[slot], out_b.at[slot], partner))
    i_xf = forward(i_x, out_i, x_cols, half_i, x_dev)
    for d in range(2):
        b_zf[d].wait_recv()
    b_y.append(send(out_b.at[far], out_b.at[far], partner))
    share(out_b, far)
    a_zf = forward(a_z, out_a, z_rows, half_a, z_dev)
    for slot in z_rows:
        share(out_a, slot)
    i_pair.wait_recv()
    i2_x = [[pass_on(out_i, pair_col, p, x_dev[d]) for p in half_i] for d in range(2)]
    for d in range(2):
        a_zf[d].wait_recv()
    share(out_a, far)
    i2_xf = forward(i2_x, out_i, other_cols, half_i, x_dev)
    a2_zf = forward(a2_z, out_a, other_rows, half_a, z_dev)
    for slot in other_rows:
        share(out_a, slot)
    for slot, copy in zip((other, *other_rows, other_far), b_y):
        copy.wait_recv()
        share(out_b, slot)
    for d in range(2):
        a2_zf[d].wait_recv()
    share(out_a, other_far)
    for copy in (*i_xf, *i2_xf, *to_sibling):
        copy.wait_recv()
    for copy in own:
        copy.wait()
    assert len(copies) == gather_copies
    for copy in copies:
        copy.wait_send()


def gather_all(a, b, i):
    rows, cols = lax.axis_size("row"), lax.axis_size("col")
    vmem = pl.BlockSpec(memory_space=pltpu.VMEM)
    anywhere = pl.BlockSpec(memory_space=pl.ANY)
    return pl.pallas_call(
        gather_kernel,
        in_specs=[vmem, vmem, vmem],
        out_specs=[anywhere] * 3,
        out_shape=[
            jax.ShapeDtypeStruct((rows, *a.shape), a.dtype),
            jax.ShapeDtypeStruct((rows, *b.shape), b.dtype),
            jax.ShapeDtypeStruct((cols, *i.shape), i.dtype),
        ],
        scratch_shapes=[
            pltpu.SemaphoreType.DMA((gather_copies,)),
            pltpu.SemaphoreType.DMA((gather_copies,)),
            pltpu.SemaphoreType.DMA((3,)),
        ],
        compiler_params=pltpu.CompilerParams(collective_id=0, has_side_effects=True),
        name="gather_all",
    )(a, b, i)


def exchange_kernel(spread_on, partial_ref, linear_ref, *refs):
    if spread_on:
        out_ref, pieces_ref, from_core, mine, landed, rounded, send_sem, recv_sem, own_sem = refs
    else:
        out_ref, from_core, mine, landed, send_sem, recv_sem = refs
    row, col = lax.axis_index("row"), lax.axis_index("col")
    h, z, k = row // 8, row // 2 % 4, row % 2
    l, x = col // 4, col % 4
    turns = ((1, 2), (1, 1), (1, 3), (0, 2), (1, 0), (0, 1), (0, 3), (0, 0))

    def row_of(turn, kk):
        return ((h + turn[0]) % 2 * 4 + (z + turn[1]) % 4) * 2 + kk

    def col_of(turn):
        return (l + turn[0]) % 2 * 4 + (x + turn[1]) % 4

    sibling = (row + 1 - 2 * k, col)
    neighbours = [sibling] + [(row_of(turn, k), col) for turn in turns[:-1]]
    if spread_on:
        neighbours += [(row, col_of(turn)) for turn in turns[:-1]]
    barrier = pltpu.get_barrier_semaphore()
    for device in neighbours:
        pl.semaphore_signal(barrier, inc=1, device_id=device, device_id_type=MESH)
    pl.semaphore_wait(barrier, len(neighbours))
    copies = []

    def send(src, dst, device):
        copy = pltpu.make_async_remote_copy(
            src_ref=src,
            dst_ref=dst,
            send_sem=send_sem.at[len(copies)],
            recv_sem=recv_sem.at[len(copies)],
            device_id=device,
            device_id_type=MESH,
        )
        copy.start()
        copies.append(copy)
        return copy

    peers = len(turns) - 1
    side = partial_ref.shape[1] // block_parts
    parts = [pl.ds(t * side, side) for t in range(block_parts)]
    crossed = [
        send(partial_ref.at[row_of(turn, 1 - k)], from_core.at[i], sibling)
        for i, turn in enumerate(turns)
    ]
    arrivals = []

    def send_on(i):
        device = (row_of(turns[i], k), col)
        arrivals.append([send(mine.at[i, p], landed.at[i, p], device) for p in parts])

    for i in range(peers):
        crossed[i].wait_recv()
        mine[i] = (partial_ref[row_of(turns[i], k)] + from_core[i]).astype(mine.dtype)
        if i > 0:
            send_on(i - 1)
    crossed[peers].wait_recv()
    send_on(peers - 1)
    spreads, own = [], []
    for t, p in enumerate(parts):
        total = partial_ref[row, p] + from_core[peers, p]
        for i in range(peers - 1, -1, -1):
            arrivals[i][t].wait_recv()
            total += landed[i, p].astype(jnp.float32)
        if spread_on:
            total = (linear_ref[p] + total) / spectrum_half
            rounded[p] = total.astype(rounded.dtype)
            out_ref[p] = total
            for turn in turns[:-1]:
                device = (row, col_of(turn))
                spreads.append(send(rounded.at[p], pieces_ref.at[col, p], device))
            own.append(pltpu.make_async_copy(rounded.at[p], pieces_ref.at[col, p], own_sem.at[t]))
            own[-1].start()
        else:
            out_ref[p] = total
    for copy in spreads:
        copy.wait_recv()
    for copy in own:
        copy.wait()
    for copy in copies:
        copy.wait_send()


def exchange(partial, linear, spread_on):
    rows, rows_dev, width = partial.shape
    cols = lax.axis_size("col")
    count = 8 + 7 * block_parts * (2 if spread_on else 1)
    vmem = pl.BlockSpec(memory_space=pltpu.VMEM)
    block = jax.ShapeDtypeStruct((rows_dev, width), jnp.float32)
    scratch = [
        pltpu.VMEM((8, rows_dev, width), jnp.float32),
        pltpu.VMEM((7, rows_dev, width), jnp.bfloat16),
        pltpu.VMEM((7, rows_dev, width), jnp.bfloat16),
    ]
    sems = [pltpu.SemaphoreType.DMA((count,)), pltpu.SemaphoreType.DMA((count,))]
    if spread_on:
        out_shape = [block, jax.ShapeDtypeStruct((cols, rows_dev, width), jnp.bfloat16)]
        out_specs = [vmem, pl.BlockSpec(memory_space=pl.ANY)]
        scratch.append(pltpu.VMEM((rows_dev, width), jnp.bfloat16))
        sems.append(pltpu.SemaphoreType.DMA((block_parts,)))
    else:
        out_shape, out_specs = block, vmem
    return pl.pallas_call(
        functools.partial(exchange_kernel, spread_on),
        in_specs=[vmem, vmem],
        out_specs=out_specs,
        out_shape=out_shape,
        scratch_shapes=scratch + sems,
        compiler_params=pltpu.CompilerParams(
            collective_id=1 if spread_on else 2,
            has_side_effects=True,
            vmem_limit_bytes=16 * 1024 * 1024,
        ),
        name="exchange_spread" if spread_on else "exchange",
    )(partial, linear)


def apply_scratch(rows, blocks_dev, spread, depth, side, width):
    return [
        pltpu.VMEM((2 * spread + 1, depth, width), jnp.float32),
        pltpu.VMEM((rows * blocks_dev, depth, width), jnp.bfloat16),
        pltpu.VMEM((rows, blocks_dev * side, depth), jnp.bfloat16),
        pltpu.SemaphoreType.DMA,
    ]


def project_and_apply(in_slots, tables, packed_a, packed_b, packed_i, blocks_dev, side):
    rows, cols = packed_a.shape[0], packed_i.shape[0]
    depth = packed_b.shape[1]
    width = packed_i.shape[2]
    spread, depth_out = cols * blocks_dev, rows * blocks_dev
    anywhere = pl.BlockSpec(memory_space=pltpu.HBM)
    grid_spec = pltpu.PrefetchScalarGridSpec(
        num_scalar_prefetch=4,
        grid=(spread,),
        in_specs=[anywhere] * 3,
        out_specs=[
            pl.BlockSpec((2, depth, side), lambda s, *refs: (s, 0, 0)),
            pl.BlockSpec((depth_out, side, width), lambda s, *refs: (0, 0, 0)),
        ],
        scratch_shapes=[
            *apply_scratch(rows, blocks_dev, spread, depth, side, width),
            pltpu.VMEM((ring, 2, depth, depth), jnp.bfloat16),
            pltpu.VMEM((ring, depth, side), jnp.bfloat16),
            pltpu.VMEM((ring, side, width), jnp.bfloat16),
            pltpu.SemaphoreType.DMA((ring, 4)),
        ],
    )
    return pl.pallas_call(
        functools.partial(build_kernel, blocks_dev, spread),
        grid_spec=grid_spec,
        out_shape=[
            jax.ShapeDtypeStruct((2 * spread, depth, side), jnp.bfloat16),
            jax.ShapeDtypeStruct((depth_out, side, width), jnp.float32),
        ],
        compiler_params=pltpu.CompilerParams(vmem_limit_bytes=49 * 1024 * 1024),
        name="project_and_apply",
    )(in_slots, *tables, packed_a, packed_b, packed_i)


def apply_again(tables, projected, pieces, packed_a, blocks_dev):
    rows = packed_a.shape[0]
    _, depth, side = projected.shape
    cols, _, width = pieces.shape
    spread, depth_out = cols * blocks_dev, rows * blocks_dev
    grid_spec = pltpu.PrefetchScalarGridSpec(
        num_scalar_prefetch=3,
        grid=(spread // apply_group,),
        in_specs=[
            pl.BlockSpec(memory_space=pltpu.HBM),
            pl.BlockSpec(pieces.shape, lambda s, *refs: (0, 0, 0)),
            pl.BlockSpec(memory_space=pltpu.HBM),
        ],
        out_specs=pl.BlockSpec((depth_out, side, width), lambda s, *refs: (0, 0, 0)),
        scratch_shapes=[
            *apply_scratch(rows, blocks_dev, spread, depth, side, width),
            pltpu.VMEM(projected.shape, jnp.bfloat16),
            pltpu.SemaphoreType.DMA((spread // apply_group,)),
        ],
    )
    return pl.pallas_call(
        functools.partial(apply_kernel_body, blocks_dev, spread),
        grid_spec=grid_spec,
        out_shape=jax.ShapeDtypeStruct((depth_out, side, width), jnp.float32),
        compiler_params=pltpu.CompilerParams(vmem_limit_bytes=49 * 1024 * 1024),
        name="apply_again",
    )(*tables, projected, pieces, packed_a)


def on_device(
    vectors, energies, intersections, coarse, fine_coarse, coarse_slot, tile_codes, tile_count
):
    rows_count = lax.axis_size("row")
    cols_count = lax.axis_size("col")
    row_id = lax.axis_index("row")
    col_id = lax.axis_index("col")
    blocks_dev, pairs_coarse, tile_side = intersections.shape
    width_vec = vectors.shape[1]
    points_col = coarse.shape[0]
    spread = cols_count * blocks_dev
    depth_out = rows_count * blocks_dev
    groups_max = (tile_codes.shape[1] + (list_group - 1) * depth_out) // list_group
    index_out = jnp.arange(depth_out, dtype=jnp.int32)
    index_in = jnp.arange(spread, dtype=jnp.int32)
    out_blocks = (
        index_out // blocks_dev * cols_count + col_id
    ) * blocks_dev + index_out % blocks_dev
    in_blocks = (row_id * cols_count + index_in // blocks_dev) * blocks_dev + index_in % blocks_dev
    in_slots = lookup(coarse_slot, lookup(fine_coarse, in_blocks))
    out_points = lookup(fine_coarse, out_blocks) - col_id * points_col
    tables = list_tables(
        tile_codes[0], tile_count[0], depth_out, spread, out_points, groups_max
    )

    pair_energy = energies.reshape(-1, 1)
    across = jnp.swapaxes(intersections, 1, 2).reshape(-1, pairs_coarse)
    packed_a, packed_b, packed_i = gather_all(
        jnp.concatenate([coarse[0, 0], across], axis=0),
        coarse[1, 0],
        jnp.concatenate(
            [intersections.reshape(-1, tile_side), vectors.astype(jnp.bfloat16)], axis=0
        ),
    )

    def linear(field):
        return pair_energy * field - spectrum_center * field

    def by_row(partial):
        return partial.reshape(rows_count, -1, width_vec)

    projected, partial = project_and_apply(
        in_slots, tables, packed_a, packed_b, packed_i, blocks_dev, tile_side
    )
    first_step, pieces = exchange(by_row(partial), linear(vectors), True)
    partial = apply_again(tables, projected, pieces, packed_a, blocks_dev)
    kernel_part = exchange(by_row(partial), vectors, False)
    second_step = 2.0 * ((linear(first_step) + kernel_part) / spectrum_half) - vectors
    return first_step, second_step


def solution(mesh):
    in_specs = (
        P(("row", "col"), None),
        P(("row", "col")),
        P(("row", "col"), None, None),
        P("col", "row", None, None),
        P(),
        P(),
        P(("row", "col"), None),
        P(("row", "col")),
    )
    out_specs = (P(("row", "col"), None), P(("row", "col"), None))
    return jax.shard_map(
        on_device, mesh=mesh, in_specs=in_specs, out_specs=out_specs, check_vma=False
    )
```

```python
import functools

import jax
import jax.numpy as jnp
from jax import lax
from jax.experimental import pallas as pl
from jax.experimental.pallas import tpu as pltpu
from jax.sharding import PartitionSpec as P

spectrum_center = 2.0
spectrum_half = 3.0
unroll_blocks = 4
apply_group = 4
list_group = 4
sum_rows = 128
ring_groups = 3
gather_copies = 54
block_parts = 3
MESH = pl.DeviceIdType.MESH


def lookup(values_table, positions):
    matches = positions[:, None] == jnp.arange(values_table.shape[0], dtype=jnp.int32)[None, :]
    return jnp.sum(jnp.where(matches, values_table[None, :], 0), axis=1)


def list_tables(codes, count, depth_out, spread, points, groups_max):
    slots = jnp.arange(codes.shape[0], dtype=jnp.int32)
    all_codes = jnp.arange(depth_out * spread, dtype=jnp.int32)
    hits = (codes[:, None] == all_codes[None, :]) & (slots < count)[:, None]
    mask = jnp.any(hits, axis=0).astype(jnp.int32).reshape(depth_out, spread)
    filled = jnp.sum(mask, axis=1)
    groups = (filled + list_group - 1) // list_group
    index_out = jnp.arange(depth_out, dtype=jnp.int32)
    index_in = jnp.arange(spread, dtype=jnp.int32)
    base = jnp.sum(jnp.where(index_out[None, :] < index_out[:, None], groups[None, :], 0), axis=1)
    rank = jnp.sum(
        jnp.where(index_in[None, None, :] < index_in[None, :, None], mask[:, None, :], 0), axis=2
    )
    place = jnp.where(mask > 0, list_group * base[:, None] + rank, -1).reshape(-1)
    product = (index_in[None, :] * 2 + points[:, None]).reshape(-1)
    spots = jnp.arange(list_group * groups_max, dtype=jnp.int32)
    found = jnp.sum(jnp.where(spots[:, None] == place[None, :], product[None, :] + 1, 0), axis=1)
    return jnp.where(found > 0, found - 1, 2 * spread), base, groups


def block_of(ref, block, blocks_dev, side):
    rows = pl.ds(pl.multiple_of(block % blocks_dev * side, side), side)
    return ref[block // blocks_dev, rows, :]


def sum_products(members_ref, base_ref, groups_ref, products_ref, sums_ref, over_out_ref, out_ref):
    depth_out, side, width = out_ref.shape
    blocks_dev = over_out_ref.shape[1] // side
    depth = products_ref.shape[1]

    def add_up(q, carry):
        start = base_ref[q]
        stop = start + groups_ref[q]
        for c in range(depth // sum_rows):
            rows = pl.ds(c * sum_rows, sum_rows)

            def add(group, total):
                parts = [
                    products_ref[members_ref[list_group * group + n], rows, :]
                    for n in range(list_group)
                ]
                while len(parts) > 1:
                    parts = [left + right for left, right in zip(parts[::2], parts[1::2])]
                return total + parts[0]

            total = lax.fori_loop(start, stop, add, jnp.zeros((sum_rows, width), jnp.float32))
            sums_ref[q, rows, :] = total.astype(sums_ref.dtype)
        return carry

    lax.fori_loop(0, depth_out, add_up, 0)

    def finish(group, carry):
        for u in range(unroll_blocks):
            q = group * unroll_blocks + u
            out_ref[q] = jnp.dot(
                block_of(over_out_ref, q, blocks_dev, side),
                sums_ref[q],
                preferred_element_type=jnp.float32,
            )
        return carry

    lax.fori_loop(0, depth_out // unroll_blocks, finish, 0)


def build_kernel(
    blocks_dev,
    spread,
    slots_ref,
    members_ref,
    base_ref,
    groups_ref,
    packed_a_ref,
    packed_b_ref,
    packed_i_ref,
    projected_ref,
    out_ref,
    products_ref,
    sums_ref,
    over_out_ref,
    sem,
    coarse_ref,
    over_in_ref,
    field_ref,
    ring_sems,
):
    step = pl.program_id(0)
    side = out_ref.shape[1]
    depth = packed_b_ref.shape[1]

    def reads(block, place):
        slot = slots_ref[block]
        owner, local = block // blocks_dev, block % blocks_dev
        over_rows = pl.ds(pl.multiple_of(local * depth, depth), depth)
        field_rows = pl.ds(pl.multiple_of(blocks_dev * depth + local * side, side), side)
        sources = (
            (packed_a_ref.at[slot, pl.ds(0, depth), :], coarse_ref.at[place, 0]),
            (packed_b_ref.at[slot], coarse_ref.at[place, 1]),
            (packed_i_ref.at[owner, over_rows, :], over_in_ref.at[place]),
            (packed_i_ref.at[owner, field_rows, :], field_ref.at[place]),
        )
        return [
            pltpu.make_async_copy(src, dst, ring_sems.at[place, n])
            for n, (src, dst) in enumerate(sources)
        ]

    copy = pltpu.make_async_copy(
        packed_a_ref.at[:, pl.ds(depth, blocks_dev * side), :], over_out_ref, sem
    )

    @pl.when(step == 0)
    def _():
        for block in range(ring_groups * blocks_dev):
            for read in reads(block, block):
                read.start()
        copy.start()
        products_ref[2 * spread] = jnp.zeros(products_ref.shape[1:], products_ref.dtype)

    first_place = step % ring_groups * blocks_dev
    for local in range(blocks_dev):
        block, place = step * blocks_dev + local, first_place + local
        for read in reads(block, place):
            read.wait()
        for a in range(2):
            projected = jnp.dot(
                coarse_ref[place, a], over_in_ref[place], preferred_element_type=jnp.float32
            ).astype(jnp.bfloat16)
            projected_ref[2 * local + a] = projected
            products_ref[block * 2 + a] = jnp.dot(
                projected, field_ref[place], preferred_element_type=jnp.float32
            )

    @pl.when(step + ring_groups < pl.num_programs(0))
    def _():
        for local in range(blocks_dev):
            for read in reads((step + ring_groups) * blocks_dev + local, first_place + local):
                read.start()

    @pl.when(step == pl.num_programs(0) - 1)
    def _():
        copy.wait()
        sum_products(
            members_ref, base_ref, groups_ref, products_ref, sums_ref, over_out_ref, out_ref
        )


def apply_kernel_body(
    blocks_dev,
    spread,
    members_ref,
    base_ref,
    groups_ref,
    projected_ref,
    pieces_ref,
    packed_a_ref,
    out_ref,
    products_ref,
    sums_ref,
    over_out_ref,
    sem,
    held_ref,
    group_sems,
):
    step = pl.program_id(0)
    side = out_ref.shape[1]
    depth = projected_ref.shape[1]
    groups = spread // apply_group
    reads = [
        pltpu.make_async_copy(
            projected_ref.at[pl.ds(2 * apply_group * g, 2 * apply_group)],
            held_ref.at[pl.ds(2 * apply_group * g, 2 * apply_group)],
            group_sems.at[g],
        )
        for g in range(groups)
    ]
    copy = pltpu.make_async_copy(
        packed_a_ref.at[:, pl.ds(depth, blocks_dev * side), :], over_out_ref, sem
    )

    @pl.when(step == 0)
    def _():
        for read in reads:
            read.start()
        copy.start()
        products_ref[2 * spread] = jnp.zeros(products_ref.shape[1:], products_ref.dtype)

    for g, read in enumerate(reads):
        pl.when(step == g)(read.wait)

    for g in range(apply_group):
        block = step * apply_group + g
        field = block_of(pieces_ref, block, blocks_dev, side)
        for a in range(2):
            products_ref[block * 2 + a] = jnp.dot(
                held_ref[block * 2 + a], field, preferred_element_type=jnp.float32
            )

    @pl.when(step == pl.num_programs(0) - 1)
    def _():
        copy.wait()
        sum_products(
            members_ref, base_ref, groups_ref, products_ref, sums_ref, over_out_ref, out_ref
        )


def gather_kernel(coarse_ref, across_ref, i_ref, out_a, out_b, out_i, send_sem, recv_sem, own_sem):
    row, col = lax.axis_index("row"), lax.axis_index("col")
    h, z, k = row // 8, row // 2 % 4, row % 2
    l, x = col // 4, col % 4

    def row_of(hh, zz):
        return (hh * 4 + zz % 4) * 2 + k

    partner = (row_of(1 - h, z), col)
    z_dev = ((row_of(h, z + 1), col), (row_of(h, z + 3), col))
    x_dev = ((row, l * 4 + (x + 1) % 4), (row, l * 4 + (x + 3) % 4))
    sibling = (row + 1 - 2 * k, col)
    pair = (row, (1 - l) * 4 + x)

    barrier = pltpu.get_barrier_semaphore()
    neighbours = (partner, *z_dev, *x_dev, sibling, pair)
    for device in neighbours:
        pl.semaphore_signal(barrier, inc=1, device_id=device, device_id_type=MESH)
    pl.semaphore_wait(barrier, len(neighbours))

    def halves(ref):
        size = ref.shape[0] // 2
        return [pl.ds(s * size, size) for s in range(2)]

    depth = coarse_ref.shape[1]
    a_own = (coarse_ref.at[0], across_ref)
    half_a = [pl.ds(0, depth), pl.ds(depth, across_ref.shape[0])]
    half_b, half_i = halves(coarse_ref.at[1]), halves(i_ref)
    copies, to_sibling = [], []

    def send(src, dst, device):
        copy = pltpu.make_async_remote_copy(
            src_ref=src,
            dst_ref=dst,
            send_sem=send_sem.at[len(copies)],
            recv_sem=recv_sem.at[len(copies)],
            device_id=device,
            device_id_type=MESH,
        )
        copy.start()
        copies.append(copy)
        return copy

    def pass_on(out, slot, part, device):
        return send(out.at[slot, part], out.at[slot, part], device)

    def share(out, slot):
        to_sibling.append(send(out.at[slot], out.at[slot], sibling))

    def forward(arrivals, out, slots, parts, devices, flip=0):
        sent = []
        for d in range(2):
            arrivals[d][d ^ flip].wait_recv()
            sent.append(pass_on(out, slots[d], parts[d ^ flip], devices[d]))
        arrivals[0][1 ^ flip].wait_recv()
        arrivals[1][flip].wait_recv()
        return sent

    a_y = [send(src, out_a.at[row, p], partner) for src, p in zip(a_own, half_a)]
    b_z = [
        [send(coarse_ref.at[1, p], out_b.at[row, p], z_dev[d]) for p in half_b] for d in range(2)
    ]
    i_x = [[send(i_ref.at[p], out_i.at[col, p], x_dev[d]) for p in half_i] for d in range(2)]
    for src, p in zip(a_own, half_a):
        to_sibling.append(send(src, out_a.at[row, p], sibling))
    to_sibling.append(send(coarse_ref.at[1], out_b.at[row], sibling))
    own = [
        pltpu.make_async_copy(a_own[0], out_a.at[row, half_a[0]], own_sem.at[0]),
        pltpu.make_async_copy(a_own[1], out_a.at[row, half_a[1]], own_sem.at[1]),
        pltpu.make_async_copy(coarse_ref.at[1], out_b.at[row], own_sem.at[2]),
        pltpu.make_async_copy(i_ref, out_i.at[col], own_sem.at[3]),
    ]
    for copy in own:
        copy.start()

    z_rows = (row_of(h, z + 3), row_of(h, z + 1))
    far = row_of(h, z + 2)
    x_cols = (l * 4 + (x + 3) % 4, l * 4 + (x + 1) % 4)
    other = row_of(1 - h, z)
    other_rows = (row_of(1 - h, z + 3), row_of(1 - h, z + 1))
    other_far = row_of(1 - h, z + 2)
    pair_col = (1 - l) * 4 + x
    other_cols = ((1 - l) * 4 + (x + 3) % 4, (1 - l) * 4 + (x + 1) % 4)

    b_zf = forward(b_z, out_b, z_rows, half_b, z_dev)
    a_z = [
        [send(src, out_a.at[row, p], z_dev[d]) for src, p in zip(a_own, half_a)] for d in range(2)
    ]
    for slot in z_rows:
        share(out_b, slot)
    a2_z = [[None, None], [None, None]]
    for s in range(2):
        a_y[s].wait_recv()
        for d in range(2):
            a2_z[d][s] = pass_on(out_a, other, half_a[s], z_dev[d])
    share(out_a, other)
    i_pair = send(i_ref, out_i.at[col], pair)
    b_y = [send(coarse_ref.at[1], out_b.at[row], partner)]
    for slot in z_rows:
        b_y.append(send(out_b.at[slot], out_b.at[slot], partner))
    i_xf = forward(i_x, out_i, x_cols, half_i, x_dev)
    for d in range(2):
        b_zf[d].wait_recv()
    b_y.append(send(out_b.at[far], out_b.at[far], partner))
    share(out_b, far)
    a_zf = forward(a_z, out_a, z_rows, half_a, z_dev)
    for slot in z_rows:
        share(out_a, slot)
    i_pair.wait_recv()
    i2_x = [[pass_on(out_i, pair_col, p, x_dev[d]) for p in half_i] for d in range(2)]
    for d in range(2):
        a_zf[d].wait_recv()
    share(out_a, far)
    i2_xf = forward(i2_x, out_i, other_cols, half_i, x_dev)
    a2_zf = forward(a2_z, out_a, other_rows, half_a, z_dev, 1)
    for slot in other_rows:
        share(out_a, slot)
    for slot, copy in zip((other, *other_rows, other_far), b_y):
        copy.wait_recv()
        share(out_b, slot)
    for d in range(2):
        a2_zf[d].wait_recv()
    share(out_a, other_far)
    for copy in (*i_xf, *i2_xf, *to_sibling):
        copy.wait_recv()
    for copy in own:
        copy.wait()
    assert len(copies) == gather_copies
    for copy in copies:
        copy.wait_send()


def gather_all(coarse, across, i):
    rows, cols = lax.axis_size("row"), lax.axis_size("col")
    depth = coarse.shape[1]
    vmem = pl.BlockSpec(memory_space=pltpu.VMEM)
    anywhere = pl.BlockSpec(memory_space=pl.ANY)
    return pl.pallas_call(
        gather_kernel,
        in_specs=[vmem, vmem, vmem],
        out_specs=[anywhere] * 3,
        out_shape=[
            jax.ShapeDtypeStruct((rows, depth + across.shape[0], depth), coarse.dtype),
            jax.ShapeDtypeStruct((rows, depth, depth), coarse.dtype),
            jax.ShapeDtypeStruct((cols, *i.shape), i.dtype),
        ],
        scratch_shapes=[
            pltpu.SemaphoreType.DMA((gather_copies,)),
            pltpu.SemaphoreType.DMA((gather_copies,)),
            pltpu.SemaphoreType.DMA((4,)),
        ],
        compiler_params=pltpu.CompilerParams(collective_id=0, has_side_effects=True),
        name="gather_all",
    )(coarse, across, i)


def exchange_kernel(spread_on, partial_ref, linear_ref, *refs):
    if spread_on:
        out_ref, pieces_ref, from_core, mine, landed, rounded, send_sem, recv_sem, own_sem = refs
    else:
        out_ref, from_core, mine, landed, send_sem, recv_sem = refs
    row, col = lax.axis_index("row"), lax.axis_index("col")
    h, z, k = row // 8, row // 2 % 4, row % 2
    l, x = col // 4, col % 4
    turns = ((1, 2), (1, 1), (1, 3), (0, 2), (1, 0), (0, 1), (0, 3), (0, 0))

    def row_of(turn, kk):
        return ((h + turn[0]) % 2 * 4 + (z + turn[1]) % 4) * 2 + kk

    def col_of(turn):
        return (l + turn[0]) % 2 * 4 + (x + turn[1]) % 4

    sibling = (row + 1 - 2 * k, col)
    neighbours = [sibling] + [(row_of(turn, k), col) for turn in turns[:-1]]
    if spread_on:
        neighbours += [(row, col_of(turn)) for turn in turns[:-1]]
    barrier = pltpu.get_barrier_semaphore()
    for device in neighbours:
        pl.semaphore_signal(barrier, inc=1, device_id=device, device_id_type=MESH)
    pl.semaphore_wait(barrier, len(neighbours))
    copies = []

    def send(src, dst, device):
        copy = pltpu.make_async_remote_copy(
            src_ref=src,
            dst_ref=dst,
            send_sem=send_sem.at[len(copies)],
            recv_sem=recv_sem.at[len(copies)],
            device_id=device,
            device_id_type=MESH,
        )
        copy.start()
        copies.append(copy)
        return copy

    peers = len(turns) - 1
    side = partial_ref.shape[1] // block_parts
    parts = [pl.ds(t * side, side) for t in range(block_parts)]
    crossed = [
        send(partial_ref.at[row_of(turn, 1 - k)], from_core.at[i], sibling)
        for i, turn in enumerate(turns)
    ]
    arrivals = []

    def send_on(i):
        device = (row_of(turns[i], k), col)
        arrivals.append([send(mine.at[i, p], landed.at[i, p], device) for p in parts])

    for i in range(peers):
        crossed[i].wait_recv()
        mine[i] = (partial_ref[row_of(turns[i], k)] + from_core[i]).astype(mine.dtype)
        if i > 0:
            send_on(i - 1)
    crossed[peers].wait_recv()
    send_on(peers - 1)
    spreads, own = [], []
    for t, p in enumerate(parts):
        total = partial_ref[row, p] + from_core[peers, p]
        for i in range(peers - 1, -1, -1):
            arrivals[i][t].wait_recv()
            total += landed[i, p].astype(jnp.float32)
        if spread_on:
            total = (linear_ref[p] + total) / spectrum_half
            rounded[p] = total.astype(rounded.dtype)
            out_ref[p] = total
            for turn in turns[:-1]:
                device = (row, col_of(turn))
                spreads.append(send(rounded.at[p], pieces_ref.at[col, p], device))
            own.append(pltpu.make_async_copy(rounded.at[p], pieces_ref.at[col, p], own_sem.at[t]))
            own[-1].start()
        else:
            out_ref[p] = total
    for copy in spreads:
        copy.wait_recv()
    for copy in own:
        copy.wait()
    for copy in copies:
        copy.wait_send()


def exchange(partial, linear, spread_on):
    rows, rows_dev, width = partial.shape
    cols = lax.axis_size("col")
    count = 8 + 7 * block_parts * (2 if spread_on else 1)
    vmem = pl.BlockSpec(memory_space=pltpu.VMEM)
    block = jax.ShapeDtypeStruct((rows_dev, width), jnp.float32)
    scratch = [
        pltpu.VMEM((8, rows_dev, width), jnp.float32),
        pltpu.VMEM((7, rows_dev, width), jnp.bfloat16),
        pltpu.VMEM((7, rows_dev, width), jnp.bfloat16),
    ]
    sems = [pltpu.SemaphoreType.DMA((count,)), pltpu.SemaphoreType.DMA((count,))]
    if spread_on:
        out_shape = [block, jax.ShapeDtypeStruct((cols, rows_dev, width), jnp.bfloat16)]
        out_specs = [vmem, pl.BlockSpec(memory_space=pl.ANY)]
        scratch.append(pltpu.VMEM((rows_dev, width), jnp.bfloat16))
        sems.append(pltpu.SemaphoreType.DMA((block_parts,)))
    else:
        out_shape, out_specs = block, vmem
    return pl.pallas_call(
        functools.partial(exchange_kernel, spread_on),
        in_specs=[vmem, vmem],
        out_specs=out_specs,
        out_shape=out_shape,
        scratch_shapes=scratch + sems,
        compiler_params=pltpu.CompilerParams(
            collective_id=1 if spread_on else 2,
            has_side_effects=True,
            vmem_limit_bytes=16 * 1024 * 1024,
        ),
        name="exchange_spread" if spread_on else "exchange",
    )(partial, linear)


def apply_scratch(rows, blocks_dev, spread, depth, side, width):
    return [
        pltpu.VMEM((2 * spread + 1, depth, width), jnp.float32),
        pltpu.VMEM((rows * blocks_dev, depth, width), jnp.bfloat16),
        pltpu.VMEM((rows, blocks_dev * side, depth), jnp.bfloat16),
        pltpu.SemaphoreType.DMA,
    ]


def project_and_apply(in_slots, tables, packed_a, packed_b, packed_i, blocks_dev, side):
    rows, cols = packed_a.shape[0], packed_i.shape[0]
    depth = packed_b.shape[1]
    width = packed_i.shape[2]
    spread, depth_out = cols * blocks_dev, rows * blocks_dev
    anywhere = pl.BlockSpec(memory_space=pltpu.HBM)
    ring = ring_groups * blocks_dev
    grid_spec = pltpu.PrefetchScalarGridSpec(
        num_scalar_prefetch=4,
        grid=(cols,),
        in_specs=[anywhere] * 3,
        out_specs=[
            pl.BlockSpec((2 * blocks_dev, depth, side), lambda s, *refs: (s, 0, 0)),
            pl.BlockSpec((depth_out, side, width), lambda s, *refs: (0, 0, 0)),
        ],
        scratch_shapes=[
            *apply_scratch(rows, blocks_dev, spread, depth, side, width),
            pltpu.VMEM((ring, 2, depth, depth), jnp.bfloat16),
            pltpu.VMEM((ring, depth, side), jnp.bfloat16),
            pltpu.VMEM((ring, side, width), jnp.bfloat16),
            pltpu.SemaphoreType.DMA((ring, 4)),
        ],
    )
    return pl.pallas_call(
        functools.partial(build_kernel, blocks_dev, spread),
        grid_spec=grid_spec,
        out_shape=[
            jax.ShapeDtypeStruct((2 * spread, depth, side), jnp.bfloat16),
            jax.ShapeDtypeStruct((depth_out, side, width), jnp.float32),
        ],
        compiler_params=pltpu.CompilerParams(vmem_limit_bytes=49 * 1024 * 1024),
        name="project_and_apply",
    )(in_slots, *tables, packed_a, packed_b, packed_i)


def apply_again(tables, projected, pieces, packed_a, blocks_dev):
    rows = packed_a.shape[0]
    _, depth, side = projected.shape
    cols, _, width = pieces.shape
    spread, depth_out = cols * blocks_dev, rows * blocks_dev
    grid_spec = pltpu.PrefetchScalarGridSpec(
        num_scalar_prefetch=3,
        grid=(spread // apply_group,),
        in_specs=[
            pl.BlockSpec(memory_space=pltpu.HBM),
            pl.BlockSpec(pieces.shape, lambda s, *refs: (0, 0, 0)),
            pl.BlockSpec(memory_space=pltpu.HBM),
        ],
        out_specs=pl.BlockSpec((depth_out, side, width), lambda s, *refs: (0, 0, 0)),
        scratch_shapes=[
            *apply_scratch(rows, blocks_dev, spread, depth, side, width),
            pltpu.VMEM(projected.shape, jnp.bfloat16),
            pltpu.SemaphoreType.DMA((spread // apply_group,)),
        ],
    )
    return pl.pallas_call(
        functools.partial(apply_kernel_body, blocks_dev, spread),
        grid_spec=grid_spec,
        out_shape=jax.ShapeDtypeStruct((depth_out, side, width), jnp.float32),
        compiler_params=pltpu.CompilerParams(vmem_limit_bytes=49 * 1024 * 1024),
        name="apply_again",
    )(*tables, projected, pieces, packed_a)


def on_device(
    vectors, energies, intersections, coarse, fine_coarse, coarse_slot, tile_codes, tile_count
):
    rows_count = lax.axis_size("row")
    cols_count = lax.axis_size("col")
    row_id = lax.axis_index("row")
    col_id = lax.axis_index("col")
    blocks_dev, pairs_coarse, tile_side = intersections.shape
    width_vec = vectors.shape[1]
    points_col = coarse.shape[0]
    spread = cols_count * blocks_dev
    depth_out = rows_count * blocks_dev
    groups_max = (tile_codes.shape[1] + (list_group - 1) * depth_out) // list_group
    index_out = jnp.arange(depth_out, dtype=jnp.int32)
    index_in = jnp.arange(spread, dtype=jnp.int32)
    out_blocks = (
        index_out // blocks_dev * cols_count + col_id
    ) * blocks_dev + index_out % blocks_dev
    in_blocks = (row_id * cols_count + index_in // blocks_dev) * blocks_dev + index_in % blocks_dev
    in_slots = lookup(coarse_slot, lookup(fine_coarse, in_blocks))
    out_points = lookup(fine_coarse, out_blocks) - col_id * points_col
    tables = list_tables(
        tile_codes[0], tile_count[0], depth_out, spread, out_points, groups_max
    )

    pair_energy = energies.reshape(-1, 1)
    across = jnp.swapaxes(intersections, 1, 2).reshape(-1, pairs_coarse)
    packed_a, packed_b, packed_i = gather_all(
        coarse[:, 0],
        across,
        jnp.concatenate(
            [intersections.reshape(-1, tile_side), vectors.astype(jnp.bfloat16)], axis=0
        ),
    )

    def linear(field):
        return pair_energy * field - spectrum_center * field

    def by_row(partial):
        return partial.reshape(rows_count, -1, width_vec)

    projected, partial = project_and_apply(
        in_slots, tables, packed_a, packed_b, packed_i, blocks_dev, tile_side
    )
    first_step, pieces = exchange(by_row(partial), linear(vectors), True)
    partial = apply_again(tables, projected, pieces, packed_a, blocks_dev)
    kernel_part = exchange(by_row(partial), vectors, False)
    second_step = 2.0 * ((linear(first_step) + kernel_part) / spectrum_half) - vectors
    return first_step, second_step


def solution(mesh):
    in_specs = (
        P(("row", "col"), None),
        P(("row", "col")),
        P(("row", "col"), None, None),
        P("col", "row", None, None),
        P(),
        P(),
        P(("row", "col"), None),
        P(("row", "col")),
    )
    out_specs = (P(("row", "col"), None), P(("row", "col"), None))
    return jax.shard_map(
        on_device, mesh=mesh, in_specs=in_specs, out_specs=out_specs, check_vma=False
    )
```

```python
import functools

import jax
import jax.numpy as jnp
from jax import lax
from jax.experimental import pallas as pl
from jax.experimental.pallas import tpu as pltpu
from jax.sharding import PartitionSpec as P

spectrum_center = 2.0
spectrum_half = 3.0
unroll_blocks = 4
apply_group = 4
list_group = 4
sum_rows = 128
ring_groups = 3
gather_copies = 54
block_parts = 3
MESH = pl.DeviceIdType.MESH


def lookup(values_table, positions):
    matches = positions[:, None] == jnp.arange(values_table.shape[0], dtype=jnp.int32)[None, :]
    return jnp.sum(jnp.where(matches, values_table[None, :], 0), axis=1)


def list_tables(codes, count, depth_out, spread, points, groups_max):
    slots = jnp.arange(codes.shape[0], dtype=jnp.int32)
    all_codes = jnp.arange(depth_out * spread, dtype=jnp.int32)
    hits = (codes[:, None] == all_codes[None, :]) & (slots < count)[:, None]
    mask = jnp.any(hits, axis=0).astype(jnp.int32).reshape(depth_out, spread)
    filled = jnp.sum(mask, axis=1)
    groups = (filled + list_group - 1) // list_group
    index_out = jnp.arange(depth_out, dtype=jnp.int32)
    index_in = jnp.arange(spread, dtype=jnp.int32)
    base = jnp.sum(jnp.where(index_out[None, :] < index_out[:, None], groups[None, :], 0), axis=1)
    rank = jnp.sum(
        jnp.where(index_in[None, None, :] < index_in[None, :, None], mask[:, None, :], 0), axis=2
    )
    place = jnp.where(mask > 0, list_group * base[:, None] + rank, -1).reshape(-1)
    product = (index_in[None, :] * 2 + points[:, None]).reshape(-1)
    spots = jnp.arange(list_group * groups_max, dtype=jnp.int32)
    found = jnp.sum(jnp.where(spots[:, None] == place[None, :], product[None, :] + 1, 0), axis=1)
    return jnp.where(found > 0, found - 1, 2 * spread), base, groups


def block_of(ref, block, blocks_dev, side):
    rows = pl.ds(pl.multiple_of(block % blocks_dev * side, side), side)
    return ref[block // blocks_dev, rows, :]


def sum_products(members_ref, base_ref, groups_ref, products_ref, sums_ref, over_out_ref, out_ref):
    depth_out, side, width = out_ref.shape
    blocks_dev = over_out_ref.shape[1] // side
    depth = products_ref.shape[1]

    def add_up(q, carry):
        start = base_ref[q]
        stop = start + groups_ref[q]
        for c in range(depth // sum_rows):
            rows = pl.ds(c * sum_rows, sum_rows)

            def add(group, total):
                parts = [
                    products_ref[members_ref[list_group * group + n], rows, :]
                    for n in range(list_group)
                ]
                while len(parts) > 1:
                    parts = [left + right for left, right in zip(parts[::2], parts[1::2])]
                return total + parts[0]

            total = lax.fori_loop(start, stop, add, jnp.zeros((sum_rows, width), jnp.float32))
            sums_ref[q, rows, :] = total.astype(sums_ref.dtype)
        return carry

    lax.fori_loop(0, depth_out, add_up, 0)

    def finish(group, carry):
        for u in range(unroll_blocks):
            q = group * unroll_blocks + u
            out_ref[q] = jnp.dot(
                block_of(over_out_ref, q, blocks_dev, side),
                sums_ref[q],
                preferred_element_type=jnp.float32,
            )
        return carry

    lax.fori_loop(0, depth_out // unroll_blocks, finish, 0)


def build_kernel(
    blocks_dev,
    spread,
    slots_ref,
    members_ref,
    base_ref,
    groups_ref,
    packed_a_ref,
    packed_b_ref,
    packed_i_ref,
    projected_ref,
    out_ref,
    products_ref,
    sums_ref,
    over_out_ref,
    sem,
    coarse_ref,
    over_in_ref,
    field_ref,
    ring_sems,
):
    step = pl.program_id(0)
    side = out_ref.shape[1]
    depth = packed_b_ref.shape[1]

    def reads(block, place):
        slot = slots_ref[block]
        owner, local = block // blocks_dev, block % blocks_dev
        over_rows = pl.ds(pl.multiple_of(local * depth, depth), depth)
        field_rows = pl.ds(pl.multiple_of(blocks_dev * depth + local * side, side), side)
        sources = (
            (packed_a_ref.at[slot, pl.ds(0, depth), :], coarse_ref.at[place, 0]),
            (packed_b_ref.at[slot], coarse_ref.at[place, 1]),
            (packed_i_ref.at[owner, over_rows, :], over_in_ref.at[place]),
            (packed_i_ref.at[owner, field_rows, :], field_ref.at[place]),
        )
        return [
            pltpu.make_async_copy(src, dst, ring_sems.at[place, n])
            for n, (src, dst) in enumerate(sources)
        ]

    copy = pltpu.make_async_copy(
        packed_a_ref.at[:, pl.ds(depth, blocks_dev * side), :], over_out_ref, sem
    )

    @pl.when(step == 0)
    def _():
        for block in range(ring_groups * blocks_dev):
            for read in reads(block, block):
                read.start()
        copy.start()
        products_ref[2 * spread] = jnp.zeros(products_ref.shape[1:], products_ref.dtype)

    first_place = step % ring_groups * blocks_dev
    for local in range(blocks_dev):
        block, place = step * blocks_dev + local, first_place + local
        for read in reads(block, place):
            read.wait()
        for a in range(2):
            projected = jnp.dot(
                coarse_ref[place, a], over_in_ref[place], preferred_element_type=jnp.float32
            ).astype(jnp.bfloat16)
            projected_ref[2 * local + a] = projected
            products_ref[block * 2 + a] = jnp.dot(
                projected, field_ref[place], preferred_element_type=jnp.float32
            )

    @pl.when(step + ring_groups < pl.num_programs(0))
    def _():
        for local in range(blocks_dev):
            for read in reads((step + ring_groups) * blocks_dev + local, first_place + local):
                read.start()

    @pl.when(step == pl.num_programs(0) - 1)
    def _():
        copy.wait()
        sum_products(
            members_ref, base_ref, groups_ref, products_ref, sums_ref, over_out_ref, out_ref
        )


def apply_kernel_body(
    blocks_dev,
    spread,
    members_ref,
    base_ref,
    groups_ref,
    projected_ref,
    pieces_ref,
    packed_a_ref,
    out_ref,
    products_ref,
    sums_ref,
    over_out_ref,
    sem,
    held_ref,
    group_sems,
):
    step = pl.program_id(0)
    side = out_ref.shape[1]
    depth = projected_ref.shape[1]
    groups = spread // apply_group
    reads = [
        pltpu.make_async_copy(
            projected_ref.at[pl.ds(2 * apply_group * g, 2 * apply_group)],
            held_ref.at[pl.ds(2 * apply_group * g, 2 * apply_group)],
            group_sems.at[g],
        )
        for g in range(groups)
    ]
    copy = pltpu.make_async_copy(
        packed_a_ref.at[:, pl.ds(depth, blocks_dev * side), :], over_out_ref, sem
    )

    @pl.when(step == 0)
    def _():
        for read in reads:
            read.start()
        copy.start()
        products_ref[2 * spread] = jnp.zeros(products_ref.shape[1:], products_ref.dtype)

    for g, read in enumerate(reads):
        pl.when(step == g)(read.wait)

    for g in range(apply_group):
        block = step * apply_group + g
        field = block_of(pieces_ref, block, blocks_dev, side)
        for a in range(2):
            products_ref[block * 2 + a] = jnp.dot(
                held_ref[block * 2 + a], field, preferred_element_type=jnp.float32
            )

    @pl.when(step == pl.num_programs(0) - 1)
    def _():
        copy.wait()
        sum_products(
            members_ref, base_ref, groups_ref, products_ref, sums_ref, over_out_ref, out_ref
        )


def gather_kernel(coarse_ref, across_ref, i_ref, out_a, out_b, out_i, send_sem, recv_sem, own_sem):
    row, col = lax.axis_index("row"), lax.axis_index("col")
    h, z, k = row // 8, row // 2 % 4, row % 2
    l, x = col // 4, col % 4

    def row_of(hh, zz):
        return (hh * 4 + zz % 4) * 2 + k

    partner = (row_of(1 - h, z), col)
    z_dev = ((row_of(h, z + 1), col), (row_of(h, z + 3), col))
    x_dev = ((row, l * 4 + (x + 1) % 4), (row, l * 4 + (x + 3) % 4))
    sibling = (row + 1 - 2 * k, col)
    pair = (row, (1 - l) * 4 + x)

    barrier = pltpu.get_barrier_semaphore()
    neighbours = (partner, *z_dev, *x_dev, sibling, pair)
    for device in neighbours:
        pl.semaphore_signal(barrier, inc=1, device_id=device, device_id_type=MESH)
    pl.semaphore_wait(barrier, len(neighbours))

    def halves(ref):
        size = ref.shape[0] // 2
        return [pl.ds(s * size, size) for s in range(2)]

    depth = coarse_ref.shape[1]
    a_own = (coarse_ref.at[0], across_ref)
    half_a = [pl.ds(0, depth), pl.ds(depth, across_ref.shape[0])]
    half_b, half_i = halves(coarse_ref.at[1]), halves(i_ref)
    copies, to_sibling = [], []

    def send(src, dst, device):
        copy = pltpu.make_async_remote_copy(
            src_ref=src,
            dst_ref=dst,
            send_sem=send_sem.at[len(copies)],
            recv_sem=recv_sem.at[len(copies)],
            device_id=device,
            device_id_type=MESH,
        )
        copy.start()
        copies.append(copy)
        return copy

    def pass_on(out, slot, part, device):
        return send(out.at[slot, part], out.at[slot, part], device)

    def share(out, slot):
        to_sibling.append(send(out.at[slot], out.at[slot], sibling))

    def forward(arrivals, out, slots, parts, devices, flip=0):
        sent = []
        for d in range(2):
            arrivals[d][d ^ flip].wait_recv()
            sent.append(pass_on(out, slots[d], parts[d ^ flip], devices[d]))
        arrivals[0][1 ^ flip].wait_recv()
        arrivals[1][flip].wait_recv()
        return sent

    a_y = [send(src, out_a.at[row, p], partner) for src, p in zip(a_own, half_a)]
    b_z = [
        [send(coarse_ref.at[1, p], out_b.at[row, p], z_dev[d]) for p in half_b] for d in range(2)
    ]
    i_x = [[send(i_ref.at[p], out_i.at[col, p], x_dev[d]) for p in half_i] for d in range(2)]
    for src, p in zip(a_own, half_a):
        to_sibling.append(send(src, out_a.at[row, p], sibling))
    to_sibling.append(send(coarse_ref.at[1], out_b.at[row], sibling))
    own = [
        pltpu.make_async_copy(a_own[0], out_a.at[row, half_a[0]], own_sem.at[0]),
        pltpu.make_async_copy(a_own[1], out_a.at[row, half_a[1]], own_sem.at[1]),
        pltpu.make_async_copy(coarse_ref.at[1], out_b.at[row], own_sem.at[2]),
        pltpu.make_async_copy(i_ref, out_i.at[col], own_sem.at[3]),
    ]
    for copy in own:
        copy.start()

    z_rows = (row_of(h, z + 3), row_of(h, z + 1))
    far = row_of(h, z + 2)
    x_cols = (l * 4 + (x + 3) % 4, l * 4 + (x + 1) % 4)
    other = row_of(1 - h, z)
    other_rows = (row_of(1 - h, z + 3), row_of(1 - h, z + 1))
    other_far = row_of(1 - h, z + 2)
    pair_col = (1 - l) * 4 + x
    other_cols = ((1 - l) * 4 + (x + 3) % 4, (1 - l) * 4 + (x + 1) % 4)

    b_zf = forward(b_z, out_b, z_rows, half_b, z_dev)
    a_z = [
        [send(src, out_a.at[row, p], z_dev[d]) for src, p in zip(a_own, half_a)] for d in range(2)
    ]
    for slot in z_rows:
        share(out_b, slot)
    a2_z = [[None, None], [None, None]]
    for s in range(2):
        a_y[s].wait_recv()
        for d in range(2):
            a2_z[d][s] = pass_on(out_a, other, half_a[s], z_dev[d])
    share(out_a, other)
    i_pair = send(i_ref, out_i.at[col], pair)
    b_y = [send(coarse_ref.at[1], out_b.at[row], partner)]
    for slot in z_rows:
        b_y.append(send(out_b.at[slot], out_b.at[slot], partner))
    i_xf = forward(i_x, out_i, x_cols, half_i, x_dev)
    for d in range(2):
        b_zf[d].wait_recv()
    b_y.append(send(out_b.at[far], out_b.at[far], partner))
    share(out_b, far)
    a_zf = forward(a_z, out_a, z_rows, half_a, z_dev)
    for slot in z_rows:
        share(out_a, slot)
    i_pair.wait_recv()
    i2_x = [[pass_on(out_i, pair_col, p, x_dev[d]) for p in half_i] for d in range(2)]
    for d in range(2):
        a_zf[d].wait_recv()
    share(out_a, far)
    i2_xf = forward(i2_x, out_i, other_cols, half_i, x_dev)
    a2_zf = forward(a2_z, out_a, other_rows, half_a, z_dev, 1)
    for slot in other_rows:
        share(out_a, slot)
    for slot, copy in zip((other, *other_rows, other_far), b_y):
        copy.wait_recv()
        share(out_b, slot)
    for d in range(2):
        a2_zf[d].wait_recv()
    share(out_a, other_far)
    for copy in (*i_xf, *i2_xf, *to_sibling):
        copy.wait_recv()
    for copy in own:
        copy.wait()
    assert len(copies) == gather_copies
    for copy in copies:
        copy.wait_send()


def gather_all(coarse, across, i):
    rows, cols = lax.axis_size("row"), lax.axis_size("col")
    depth = coarse.shape[1]
    vmem = pl.BlockSpec(memory_space=pltpu.VMEM)
    anywhere = pl.BlockSpec(memory_space=pl.ANY)
    return pl.pallas_call(
        gather_kernel,
        in_specs=[vmem, vmem, vmem],
        out_specs=[anywhere] * 3,
        out_shape=[
            jax.ShapeDtypeStruct((rows, depth + across.shape[0], depth), coarse.dtype),
            jax.ShapeDtypeStruct((rows, depth, depth), coarse.dtype),
            jax.ShapeDtypeStruct((cols, *i.shape), i.dtype),
        ],
        scratch_shapes=[
            pltpu.SemaphoreType.DMA((gather_copies,)),
            pltpu.SemaphoreType.DMA((gather_copies,)),
            pltpu.SemaphoreType.DMA((4,)),
        ],
        compiler_params=pltpu.CompilerParams(collective_id=0, has_side_effects=True),
        name="gather_all",
    )(coarse, across, i)


def exchange_kernel(spread_on, partial_ref, linear_ref, *refs):
    if spread_on:
        out_ref, pieces_ref, from_core, mine, landed, rounded, send_sem, recv_sem, own_sem = refs
    else:
        out_ref, from_core, mine, landed, send_sem, recv_sem = refs
    row, col = lax.axis_index("row"), lax.axis_index("col")
    h, z, k = row // 8, row // 2 % 4, row % 2
    l, x = col // 4, col % 4
    turns = ((1, 2), (1, 1), (1, 3), (0, 2), (1, 0), (0, 1), (0, 3), (0, 0))

    def row_of(turn, kk):
        return ((h + turn[0]) % 2 * 4 + (z + turn[1]) % 4) * 2 + kk

    def col_of(turn):
        return (l + turn[0]) % 2 * 4 + (x + turn[1]) % 4

    sibling = (row + 1 - 2 * k, col)
    neighbours = [sibling] + [(row_of(turn, k), col) for turn in turns[:-1]]
    if spread_on:
        neighbours += [(row, col_of(turn)) for turn in turns[:-1]]
    barrier = pltpu.get_barrier_semaphore()
    for device in neighbours:
        pl.semaphore_signal(barrier, inc=1, device_id=device, device_id_type=MESH)
    pl.semaphore_wait(barrier, len(neighbours))
    copies = []

    def send(src, dst, device):
        copy = pltpu.make_async_remote_copy(
            src_ref=src,
            dst_ref=dst,
            send_sem=send_sem.at[len(copies)],
            recv_sem=recv_sem.at[len(copies)],
            device_id=device,
            device_id_type=MESH,
        )
        copy.start()
        copies.append(copy)
        return copy

    peers = len(turns) - 1
    side = partial_ref.shape[1] // block_parts
    parts = [pl.ds(t * side, side) for t in range(block_parts)]
    crossed = [
        [
            send(partial_ref.at[row_of(turn, 1 - k), p], from_core.at[i, p], sibling)
            for i, turn in enumerate(turns)
        ]
        for p in parts
    ]
    arrivals, ready = [[] for _ in parts], []

    def send_on(t, i):
        device = (row_of(turns[i], k), col)
        arrivals[t].append(send(mine.at[i, parts[t]], landed.at[i, parts[t]], device))

    for t, p in enumerate(parts):
        for i in range(peers):
            crossed[t][i].wait_recv()
            mine[i, p] = (partial_ref[row_of(turns[i], k), p] + from_core[i, p]).astype(mine.dtype)
            if ready:
                send_on(*ready.pop())
            ready.append((t, i))
        crossed[t][peers].wait_recv()
    send_on(*ready.pop())
    spreads, own = [], []
    for t, p in enumerate(parts):
        total = partial_ref[row, p] + from_core[peers, p]
        for i in range(peers - 1, -1, -1):
            arrivals[t][i].wait_recv()
            total += landed[i, p].astype(jnp.float32)
        if spread_on:
            total = (linear_ref[p] + total) / spectrum_half
            rounded[p] = total.astype(rounded.dtype)
            out_ref[p] = total
            for turn in turns[:-1]:
                device = (row, col_of(turn))
                spreads.append(send(rounded.at[p], pieces_ref.at[col, p], device))
            own.append(pltpu.make_async_copy(rounded.at[p], pieces_ref.at[col, p], own_sem.at[t]))
            own[-1].start()
        else:
            out_ref[p] = total
    for copy in spreads:
        copy.wait_recv()
    for copy in own:
        copy.wait()
    for copy in copies:
        copy.wait_send()


def exchange(partial, linear, spread_on):
    rows, rows_dev, width = partial.shape
    cols = lax.axis_size("col")
    count = block_parts * (8 + 7 * (2 if spread_on else 1))
    vmem = pl.BlockSpec(memory_space=pltpu.VMEM)
    block = jax.ShapeDtypeStruct((rows_dev, width), jnp.float32)
    scratch = [
        pltpu.VMEM((8, rows_dev, width), jnp.float32),
        pltpu.VMEM((7, rows_dev, width), jnp.bfloat16),
        pltpu.VMEM((7, rows_dev, width), jnp.bfloat16),
    ]
    sems = [pltpu.SemaphoreType.DMA((count,)), pltpu.SemaphoreType.DMA((count,))]
    if spread_on:
        out_shape = [block, jax.ShapeDtypeStruct((cols, rows_dev, width), jnp.bfloat16)]
        out_specs = [vmem, pl.BlockSpec(memory_space=pl.ANY)]
        scratch.append(pltpu.VMEM((rows_dev, width), jnp.bfloat16))
        sems.append(pltpu.SemaphoreType.DMA((block_parts,)))
    else:
        out_shape, out_specs = block, vmem
    return pl.pallas_call(
        functools.partial(exchange_kernel, spread_on),
        in_specs=[vmem, vmem],
        out_specs=out_specs,
        out_shape=out_shape,
        scratch_shapes=scratch + sems,
        compiler_params=pltpu.CompilerParams(
            collective_id=1 if spread_on else 2,
            has_side_effects=True,
            vmem_limit_bytes=16 * 1024 * 1024,
        ),
        name="exchange_spread" if spread_on else "exchange",
    )(partial, linear)


def apply_scratch(rows, blocks_dev, spread, depth, side, width):
    return [
        pltpu.VMEM((2 * spread + 1, depth, width), jnp.float32),
        pltpu.VMEM((rows * blocks_dev, depth, width), jnp.bfloat16),
        pltpu.VMEM((rows, blocks_dev * side, depth), jnp.bfloat16),
        pltpu.SemaphoreType.DMA,
    ]


def project_and_apply(in_slots, tables, packed_a, packed_b, packed_i, blocks_dev, side):
    rows, cols = packed_a.shape[0], packed_i.shape[0]
    depth = packed_b.shape[1]
    width = packed_i.shape[2]
    spread, depth_out = cols * blocks_dev, rows * blocks_dev
    anywhere = pl.BlockSpec(memory_space=pltpu.HBM)
    ring = ring_groups * blocks_dev
    grid_spec = pltpu.PrefetchScalarGridSpec(
        num_scalar_prefetch=4,
        grid=(cols,),
        in_specs=[anywhere] * 3,
        out_specs=[
            pl.BlockSpec((2 * blocks_dev, depth, side), lambda s, *refs: (s, 0, 0)),
            pl.BlockSpec((depth_out, side, width), lambda s, *refs: (0, 0, 0)),
        ],
        scratch_shapes=[
            *apply_scratch(rows, blocks_dev, spread, depth, side, width),
            pltpu.VMEM((ring, 2, depth, depth), jnp.bfloat16),
            pltpu.VMEM((ring, depth, side), jnp.bfloat16),
            pltpu.VMEM((ring, side, width), jnp.bfloat16),
            pltpu.SemaphoreType.DMA((ring, 4)),
        ],
    )
    return pl.pallas_call(
        functools.partial(build_kernel, blocks_dev, spread),
        grid_spec=grid_spec,
        out_shape=[
            jax.ShapeDtypeStruct((2 * spread, depth, side), jnp.bfloat16),
            jax.ShapeDtypeStruct((depth_out, side, width), jnp.float32),
        ],
        compiler_params=pltpu.CompilerParams(vmem_limit_bytes=49 * 1024 * 1024),
        name="project_and_apply",
    )(in_slots, *tables, packed_a, packed_b, packed_i)


def apply_again(tables, projected, pieces, packed_a, blocks_dev):
    rows = packed_a.shape[0]
    _, depth, side = projected.shape
    cols, _, width = pieces.shape
    spread, depth_out = cols * blocks_dev, rows * blocks_dev
    grid_spec = pltpu.PrefetchScalarGridSpec(
        num_scalar_prefetch=3,
        grid=(spread // apply_group,),
        in_specs=[
            pl.BlockSpec(memory_space=pltpu.HBM),
            pl.BlockSpec(pieces.shape, lambda s, *refs: (0, 0, 0)),
            pl.BlockSpec(memory_space=pltpu.HBM),
        ],
        out_specs=pl.BlockSpec((depth_out, side, width), lambda s, *refs: (0, 0, 0)),
        scratch_shapes=[
            *apply_scratch(rows, blocks_dev, spread, depth, side, width),
            pltpu.VMEM(projected.shape, jnp.bfloat16),
            pltpu.SemaphoreType.DMA((spread // apply_group,)),
        ],
    )
    return pl.pallas_call(
        functools.partial(apply_kernel_body, blocks_dev, spread),
        grid_spec=grid_spec,
        out_shape=jax.ShapeDtypeStruct((depth_out, side, width), jnp.float32),
        compiler_params=pltpu.CompilerParams(vmem_limit_bytes=49 * 1024 * 1024),
        name="apply_again",
    )(*tables, projected, pieces, packed_a)


def on_device(
    vectors, energies, intersections, coarse, fine_coarse, coarse_slot, tile_codes, tile_count
):
    rows_count = lax.axis_size("row")
    cols_count = lax.axis_size("col")
    row_id = lax.axis_index("row")
    col_id = lax.axis_index("col")
    blocks_dev, pairs_coarse, tile_side = intersections.shape
    width_vec = vectors.shape[1]
    points_col = coarse.shape[0]
    spread = cols_count * blocks_dev
    depth_out = rows_count * blocks_dev
    groups_max = (tile_codes.shape[1] + (list_group - 1) * depth_out) // list_group
    index_out = jnp.arange(depth_out, dtype=jnp.int32)
    index_in = jnp.arange(spread, dtype=jnp.int32)
    out_blocks = (
        index_out // blocks_dev * cols_count + col_id
    ) * blocks_dev + index_out % blocks_dev
    in_blocks = (row_id * cols_count + index_in // blocks_dev) * blocks_dev + index_in % blocks_dev
    in_slots = lookup(coarse_slot, lookup(fine_coarse, in_blocks))
    out_points = lookup(fine_coarse, out_blocks) - col_id * points_col
    tables = list_tables(
        tile_codes[0], tile_count[0], depth_out, spread, out_points, groups_max
    )

    pair_energy = energies.reshape(-1, 1)
    across = jnp.swapaxes(intersections, 1, 2).reshape(-1, pairs_coarse)
    packed_a, packed_b, packed_i = gather_all(
        coarse[:, 0],
        across,
        jnp.concatenate(
            [intersections.reshape(-1, tile_side), vectors.astype(jnp.bfloat16)], axis=0
        ),
    )

    def linear(field):
        return pair_energy * field - spectrum_center * field

    def by_row(partial):
        return partial.reshape(rows_count, -1, width_vec)

    projected, partial = project_and_apply(
        in_slots, tables, packed_a, packed_b, packed_i, blocks_dev, tile_side
    )
    first_step, pieces = exchange(by_row(partial), linear(vectors), True)
    partial = apply_again(tables, projected, pieces, packed_a, blocks_dev)
    kernel_part = exchange(by_row(partial), vectors, False)
    second_step = 2.0 * ((linear(first_step) + kernel_part) / spectrum_half) - vectors
    return first_step, second_step


def solution(mesh):
    in_specs = (
        P(("row", "col"), None),
        P(("row", "col")),
        P(("row", "col"), None, None),
        P("col", "row", None, None),
        P(),
        P(),
        P(("row", "col"), None),
        P(("row", "col")),
    )
    out_specs = (P(("row", "col"), None), P(("row", "col"), None))
    return jax.shard_map(
        on_device, mesh=mesh, in_specs=in_specs, out_specs=out_specs, check_vma=False
    )
```

```python
import functools

import jax
import jax.numpy as jnp
from jax import lax
from jax.experimental import pallas as pl
from jax.experimental.pallas import tpu as pltpu
from jax.sharding import PartitionSpec as P

spectrum_center = 2.0
spectrum_half = 3.0
unroll_blocks = 8
apply_group = 8
list_group = 4
sum_rows = 128
ring_groups = 3
gather_copies = 54
block_parts = 3
MESH = pl.DeviceIdType.MESH


def lookup(values_table, positions):
    matches = positions[:, None] == jnp.arange(values_table.shape[0], dtype=jnp.int32)[None, :]
    return jnp.sum(jnp.where(matches, values_table[None, :], 0), axis=1)


def list_tables(codes, count, depth_out, spread, points, groups_max):
    slots = jnp.arange(codes.shape[0], dtype=jnp.int32)
    all_codes = jnp.arange(depth_out * spread, dtype=jnp.int32)
    hits = (codes[:, None] == all_codes[None, :]) & (slots < count)[:, None]
    mask = jnp.any(hits, axis=0).astype(jnp.int32).reshape(depth_out, spread)
    filled = jnp.sum(mask, axis=1)
    groups = (filled + list_group - 1) // list_group
    index_out = jnp.arange(depth_out, dtype=jnp.int32)
    index_in = jnp.arange(spread, dtype=jnp.int32)
    base = jnp.sum(jnp.where(index_out[None, :] < index_out[:, None], groups[None, :], 0), axis=1)
    rank = jnp.sum(
        jnp.where(index_in[None, None, :] < index_in[None, :, None], mask[:, None, :], 0), axis=2
    )
    place = jnp.where(mask > 0, list_group * base[:, None] + rank, -1).reshape(-1)
    product = (index_in[None, :] * 2 + points[:, None]).reshape(-1)
    spots = jnp.arange(list_group * groups_max, dtype=jnp.int32)
    found = jnp.sum(jnp.where(spots[:, None] == place[None, :], product[None, :] + 1, 0), axis=1)
    return jnp.where(found > 0, found - 1, 2 * spread), base, groups


def block_of(ref, block, blocks_dev, side):
    rows = pl.ds(pl.multiple_of(block % blocks_dev * side, side), side)
    return ref[block // blocks_dev, rows, :]


def sum_products(members_ref, base_ref, groups_ref, products_ref, sums_ref, over_out_ref, out_ref):
    depth_out, side, width = out_ref.shape
    blocks_dev = over_out_ref.shape[1] // side
    depth = products_ref.shape[1]

    def add_up(q, carry):
        start = base_ref[q]
        stop = start + groups_ref[q]
        for c in range(depth // sum_rows):
            rows = pl.ds(c * sum_rows, sum_rows)

            def add(group, total):
                parts = [
                    products_ref[members_ref[list_group * group + n], rows, :]
                    for n in range(list_group)
                ]
                while len(parts) > 1:
                    parts = [left + right for left, right in zip(parts[::2], parts[1::2])]
                return total + parts[0]

            total = lax.fori_loop(start, stop, add, jnp.zeros((sum_rows, width), jnp.float32))
            sums_ref[q, rows, :] = total.astype(sums_ref.dtype)
        return carry

    lax.fori_loop(0, depth_out, add_up, 0)

    def finish(group, carry):
        for u in range(unroll_blocks):
            q = group * unroll_blocks + u
            out_ref[q] = jnp.dot(
                block_of(over_out_ref, q, blocks_dev, side),
                sums_ref[q],
                preferred_element_type=jnp.float32,
            )
        return carry

    lax.fori_loop(0, depth_out // unroll_blocks, finish, 0)


def build_kernel(
    blocks_dev,
    spread,
    slots_ref,
    members_ref,
    base_ref,
    groups_ref,
    packed_a_ref,
    packed_b_ref,
    packed_i_ref,
    projected_ref,
    out_ref,
    products_ref,
    sums_ref,
    over_out_ref,
    sem,
    coarse_ref,
    over_in_ref,
    field_ref,
    ring_sems,
):
    step = pl.program_id(0)
    side = out_ref.shape[1]
    depth = packed_b_ref.shape[1]

    def reads(block, place):
        slot = slots_ref[block]
        owner, local = block // blocks_dev, block % blocks_dev
        over_rows = pl.ds(pl.multiple_of(local * depth, depth), depth)
        field_rows = pl.ds(pl.multiple_of(blocks_dev * depth + local * side, side), side)
        sources = (
            (packed_a_ref.at[slot, pl.ds(0, depth), :], coarse_ref.at[place, 0]),
            (packed_b_ref.at[slot], coarse_ref.at[place, 1]),
            (packed_i_ref.at[owner, over_rows, :], over_in_ref.at[place]),
            (packed_i_ref.at[owner, field_rows, :], field_ref.at[place]),
        )
        return [
            pltpu.make_async_copy(src, dst, ring_sems.at[place, n])
            for n, (src, dst) in enumerate(sources)
        ]

    copy = pltpu.make_async_copy(
        packed_a_ref.at[:, pl.ds(depth, blocks_dev * side), :], over_out_ref, sem
    )

    @pl.when(step == 0)
    def _():
        for block in range(ring_groups * blocks_dev):
            for read in reads(block, block):
                read.start()
        copy.start()
        products_ref[2 * spread] = jnp.zeros(products_ref.shape[1:], products_ref.dtype)

    first_place = step % ring_groups * blocks_dev
    for local in range(blocks_dev):
        block, place = step * blocks_dev + local, first_place + local
        for read in reads(block, place):
            read.wait()
        for a in range(2):
            projected = jnp.dot(
                coarse_ref[place, a], over_in_ref[place], preferred_element_type=jnp.float32
            ).astype(jnp.bfloat16)
            projected_ref[2 * local + a] = projected
            products_ref[block * 2 + a] = jnp.dot(
                projected, field_ref[place], preferred_element_type=jnp.float32
            )

    @pl.when(step + ring_groups < pl.num_programs(0))
    def _():
        for local in range(blocks_dev):
            for read in reads((step + ring_groups) * blocks_dev + local, first_place + local):
                read.start()

    @pl.when(step == pl.num_programs(0) - 1)
    def _():
        copy.wait()
        sum_products(
            members_ref, base_ref, groups_ref, products_ref, sums_ref, over_out_ref, out_ref
        )


def apply_kernel_body(
    blocks_dev,
    spread,
    members_ref,
    base_ref,
    groups_ref,
    projected_ref,
    pieces_ref,
    packed_a_ref,
    out_ref,
    products_ref,
    sums_ref,
    over_out_ref,
    sem,
    held_ref,
    group_sems,
):
    step = pl.program_id(0)
    side = out_ref.shape[1]
    depth = projected_ref.shape[1]
    groups = spread // apply_group
    reads = [
        pltpu.make_async_copy(
            projected_ref.at[pl.ds(2 * apply_group * g, 2 * apply_group)],
            held_ref.at[pl.ds(2 * apply_group * g, 2 * apply_group)],
            group_sems.at[g],
        )
        for g in range(groups)
    ]
    copy = pltpu.make_async_copy(
        packed_a_ref.at[:, pl.ds(depth, blocks_dev * side), :], over_out_ref, sem
    )

    @pl.when(step == 0)
    def _():
        for read in reads:
            read.start()
        copy.start()
        products_ref[2 * spread] = jnp.zeros(products_ref.shape[1:], products_ref.dtype)

    for g, read in enumerate(reads):
        pl.when(step == g)(read.wait)

    for g in range(apply_group):
        block = step * apply_group + g
        field = block_of(pieces_ref, block, blocks_dev, side)
        for a in range(2):
            products_ref[block * 2 + a] = jnp.dot(
                held_ref[block * 2 + a], field, preferred_element_type=jnp.float32
            )

    @pl.when(step == pl.num_programs(0) - 1)
    def _():
        copy.wait()
        sum_products(
            members_ref, base_ref, groups_ref, products_ref, sums_ref, over_out_ref, out_ref
        )


def gather_kernel(coarse_ref, across_ref, i_ref, out_a, out_b, out_i, send_sem, recv_sem, own_sem):
    row, col = lax.axis_index("row"), lax.axis_index("col")
    h, z, k = row // 8, row // 2 % 4, row % 2
    l, x = col // 4, col % 4

    def row_of(hh, zz):
        return (hh * 4 + zz % 4) * 2 + k

    partner = (row_of(1 - h, z), col)
    z_dev = ((row_of(h, z + 1), col), (row_of(h, z + 3), col))
    x_dev = ((row, l * 4 + (x + 1) % 4), (row, l * 4 + (x + 3) % 4))
    sibling = (row + 1 - 2 * k, col)
    pair = (row, (1 - l) * 4 + x)

    barrier = pltpu.get_barrier_semaphore()
    neighbours = (partner, *z_dev, *x_dev, sibling, pair)
    for device in neighbours:
        pl.semaphore_signal(barrier, inc=1, device_id=device, device_id_type=MESH)
    pl.semaphore_wait(barrier, len(neighbours))

    def halves(ref):
        size = ref.shape[0] // 2
        return [pl.ds(s * size, size) for s in range(2)]

    depth = coarse_ref.shape[1]
    a_own = (coarse_ref.at[0], across_ref)
    half_a = [pl.ds(0, depth), pl.ds(depth, across_ref.shape[0])]
    half_b, half_i = halves(coarse_ref.at[1]), halves(i_ref)
    copies, to_sibling = [], []

    def send(src, dst, device):
        copy = pltpu.make_async_remote_copy(
            src_ref=src,
            dst_ref=dst,
            send_sem=send_sem.at[len(copies)],
            recv_sem=recv_sem.at[len(copies)],
            device_id=device,
            device_id_type=MESH,
        )
        copy.start()
        copies.append(copy)
        return copy

    def pass_on(out, slot, part, device):
        return send(out.at[slot, part], out.at[slot, part], device)

    def share(out, slot):
        to_sibling.append(send(out.at[slot], out.at[slot], sibling))

    def forward(arrivals, out, slots, parts, devices, flip=0):
        sent = []
        for d in range(2):
            arrivals[d][d ^ flip].wait_recv()
            sent.append(pass_on(out, slots[d], parts[d ^ flip], devices[d]))
        arrivals[0][1 ^ flip].wait_recv()
        arrivals[1][flip].wait_recv()
        return sent

    a_y = [send(src, out_a.at[row, p], partner) for src, p in zip(a_own, half_a)]
    b_z = [
        [send(coarse_ref.at[1, p], out_b.at[row, p], z_dev[d]) for p in half_b] for d in range(2)
    ]
    i_x = [[send(i_ref.at[p], out_i.at[col, p], x_dev[d]) for p in half_i] for d in range(2)]
    for src, p in zip(a_own, half_a):
        to_sibling.append(send(src, out_a.at[row, p], sibling))
    to_sibling.append(send(coarse_ref.at[1], out_b.at[row], sibling))
    own = [
        pltpu.make_async_copy(a_own[0], out_a.at[row, half_a[0]], own_sem.at[0]),
        pltpu.make_async_copy(a_own[1], out_a.at[row, half_a[1]], own_sem.at[1]),
        pltpu.make_async_copy(coarse_ref.at[1], out_b.at[row], own_sem.at[2]),
        pltpu.make_async_copy(i_ref, out_i.at[col], own_sem.at[3]),
    ]
    for copy in own:
        copy.start()

    z_rows = (row_of(h, z + 3), row_of(h, z + 1))
    far = row_of(h, z + 2)
    x_cols = (l * 4 + (x + 3) % 4, l * 4 + (x + 1) % 4)
    other = row_of(1 - h, z)
    other_rows = (row_of(1 - h, z + 3), row_of(1 - h, z + 1))
    other_far = row_of(1 - h, z + 2)
    pair_col = (1 - l) * 4 + x
    other_cols = ((1 - l) * 4 + (x + 3) % 4, (1 - l) * 4 + (x + 1) % 4)

    b_zf = forward(b_z, out_b, z_rows, half_b, z_dev)
    a_z = [
        [send(src, out_a.at[row, p], z_dev[d]) for src, p in zip(a_own, half_a)] for d in range(2)
    ]
    for slot in z_rows:
        share(out_b, slot)
    a2_z = [[None, None], [None, None]]
    for s in range(2):
        a_y[s].wait_recv()
        for d in range(2):
            a2_z[d][s] = pass_on(out_a, other, half_a[s], z_dev[d])
    share(out_a, other)
    i_pair = send(i_ref, out_i.at[col], pair)
    b_y = [send(coarse_ref.at[1], out_b.at[row], partner)]
    for slot in z_rows:
        b_y.append(send(out_b.at[slot], out_b.at[slot], partner))
    i_xf = forward(i_x, out_i, x_cols, half_i, x_dev)
    for d in range(2):
        b_zf[d].wait_recv()
    b_y.append(send(out_b.at[far], out_b.at[far], partner))
    share(out_b, far)
    a_zf = forward(a_z, out_a, z_rows, half_a, z_dev)
    for slot in z_rows:
        share(out_a, slot)
    i_pair.wait_recv()
    i2_x = [[pass_on(out_i, pair_col, p, x_dev[d]) for p in half_i] for d in range(2)]
    for d in range(2):
        a_zf[d].wait_recv()
    share(out_a, far)
    i2_xf = forward(i2_x, out_i, other_cols, half_i, x_dev)
    a2_zf = forward(a2_z, out_a, other_rows, half_a, z_dev, 1)
    for slot in other_rows:
        share(out_a, slot)
    for slot, copy in zip((other, *other_rows, other_far), b_y):
        copy.wait_recv()
        share(out_b, slot)
    for d in range(2):
        a2_zf[d].wait_recv()
    share(out_a, other_far)
    for copy in (*i_xf, *i2_xf, *to_sibling):
        copy.wait_recv()
    for copy in own:
        copy.wait()
    assert len(copies) == gather_copies
    for copy in copies:
        copy.wait_send()


def gather_all(coarse, across, i):
    rows, cols = lax.axis_size("row"), lax.axis_size("col")
    depth = coarse.shape[1]
    vmem = pl.BlockSpec(memory_space=pltpu.VMEM)
    anywhere = pl.BlockSpec(memory_space=pl.ANY)
    return pl.pallas_call(
        gather_kernel,
        in_specs=[vmem, vmem, vmem],
        out_specs=[anywhere] * 3,
        out_shape=[
            jax.ShapeDtypeStruct((rows, depth + across.shape[0], depth), coarse.dtype),
            jax.ShapeDtypeStruct((rows, depth, depth), coarse.dtype),
            jax.ShapeDtypeStruct((cols, *i.shape), i.dtype),
        ],
        scratch_shapes=[
            pltpu.SemaphoreType.DMA((gather_copies,)),
            pltpu.SemaphoreType.DMA((gather_copies,)),
            pltpu.SemaphoreType.DMA((4,)),
        ],
        compiler_params=pltpu.CompilerParams(collective_id=0, has_side_effects=True),
        name="gather_all",
    )(coarse, across, i)


def exchange_kernel(spread_on, partial_ref, linear_ref, *refs):
    if spread_on:
        out_ref, pieces_ref, from_core, mine, landed, rounded, send_sem, recv_sem, own_sem = refs
    else:
        out_ref, from_core, mine, landed, send_sem, recv_sem = refs
    row, col = lax.axis_index("row"), lax.axis_index("col")
    h, z, k = row // 8, row // 2 % 4, row % 2
    l, x = col // 4, col % 4
    turns = ((1, 2), (1, 1), (1, 3), (0, 2), (1, 0), (0, 1), (0, 3), (0, 0))

    def row_of(turn, kk):
        return ((h + turn[0]) % 2 * 4 + (z + turn[1]) % 4) * 2 + kk

    def col_of(turn):
        return (l + turn[0]) % 2 * 4 + (x + turn[1]) % 4

    sibling = (row + 1 - 2 * k, col)
    neighbours = [sibling] + [(row_of(turn, k), col) for turn in turns[:-1]]
    if spread_on:
        neighbours += [(row, col_of(turn)) for turn in turns[:-1]]
    barrier = pltpu.get_barrier_semaphore()
    for device in neighbours:
        pl.semaphore_signal(barrier, inc=1, device_id=device, device_id_type=MESH)
    pl.semaphore_wait(barrier, len(neighbours))
    copies = []

    def send(src, dst, device):
        copy = pltpu.make_async_remote_copy(
            src_ref=src,
            dst_ref=dst,
            send_sem=send_sem.at[len(copies)],
            recv_sem=recv_sem.at[len(copies)],
            device_id=device,
            device_id_type=MESH,
        )
        copy.start()
        copies.append(copy)
        return copy

    peers = len(turns) - 1
    side = partial_ref.shape[1] // block_parts
    parts = [pl.ds(t * side, side) for t in range(block_parts)]
    crossed = [
        send(partial_ref.at[row_of(turn, 1 - k)], from_core.at[i], sibling)
        for i, turn in enumerate(turns)
    ]
    arrivals = []

    def send_on(i):
        device = (row_of(turns[i], k), col)
        arrivals.append([send(mine.at[i, p], landed.at[i, p], device) for p in parts])

    for i in range(peers):
        crossed[i].wait_recv()
        mine[i] = (partial_ref[row_of(turns[i], k)] + from_core[i]).astype(mine.dtype)
        if i > 0:
            send_on(i - 1)
    crossed[peers].wait_recv()
    send_on(peers - 1)
    spreads, own = [], []
    for t, p in enumerate(parts):
        total = partial_ref[row, p] + from_core[peers, p]
        for i in range(peers - 1, -1, -1):
            arrivals[i][t].wait_recv()
            total += landed[i, p].astype(jnp.float32)
        if spread_on:
            total = (linear_ref[p] + total) / spectrum_half
            rounded[p] = total.astype(rounded.dtype)
            out_ref[p] = total
            for turn in turns[:-1]:
                device = (row, col_of(turn))
                spreads.append(send(rounded.at[p], pieces_ref.at[col, p], device))
            own.append(pltpu.make_async_copy(rounded.at[p], pieces_ref.at[col, p], own_sem.at[t]))
            own[-1].start()
        else:
            out_ref[p] = total
    for copy in spreads:
        copy.wait_recv()
    for copy in own:
        copy.wait()
    for copy in copies:
        copy.wait_send()


def exchange(partial, linear, spread_on):
    rows, rows_dev, width = partial.shape
    cols = lax.axis_size("col")
    count = 8 + 7 * block_parts * (2 if spread_on else 1)
    vmem = pl.BlockSpec(memory_space=pltpu.VMEM)
    block = jax.ShapeDtypeStruct((rows_dev, width), jnp.float32)
    scratch = [
        pltpu.VMEM((8, rows_dev, width), jnp.float32),
        pltpu.VMEM((7, rows_dev, width), jnp.bfloat16),
        pltpu.VMEM((7, rows_dev, width), jnp.bfloat16),
    ]
    sems = [pltpu.SemaphoreType.DMA((count,)), pltpu.SemaphoreType.DMA((count,))]
    if spread_on:
        out_shape = [block, jax.ShapeDtypeStruct((cols, rows_dev, width), jnp.bfloat16)]
        out_specs = [vmem, pl.BlockSpec(memory_space=pl.ANY)]
        scratch.append(pltpu.VMEM((rows_dev, width), jnp.bfloat16))
        sems.append(pltpu.SemaphoreType.DMA((block_parts,)))
    else:
        out_shape, out_specs = block, vmem
    return pl.pallas_call(
        functools.partial(exchange_kernel, spread_on),
        in_specs=[vmem, vmem],
        out_specs=out_specs,
        out_shape=out_shape,
        scratch_shapes=scratch + sems,
        compiler_params=pltpu.CompilerParams(
            collective_id=1 if spread_on else 2,
            has_side_effects=True,
            vmem_limit_bytes=16 * 1024 * 1024,
        ),
        name="exchange_spread" if spread_on else "exchange",
    )(partial, linear)


def apply_scratch(rows, blocks_dev, spread, depth, side, width):
    return [
        pltpu.VMEM((2 * spread + 1, depth, width), jnp.float32),
        pltpu.VMEM((rows * blocks_dev, depth, width), jnp.bfloat16),
        pltpu.VMEM((rows, blocks_dev * side, depth), jnp.bfloat16),
        pltpu.SemaphoreType.DMA,
    ]


def project_and_apply(in_slots, tables, packed_a, packed_b, packed_i, blocks_dev, side):
    rows, cols = packed_a.shape[0], packed_i.shape[0]
    depth = packed_b.shape[1]
    width = packed_i.shape[2]
    spread, depth_out = cols * blocks_dev, rows * blocks_dev
    anywhere = pl.BlockSpec(memory_space=pltpu.HBM)
    ring = ring_groups * blocks_dev
    grid_spec = pltpu.PrefetchScalarGridSpec(
        num_scalar_prefetch=4,
        grid=(cols,),
        in_specs=[anywhere] * 3,
        out_specs=[
            pl.BlockSpec((2 * blocks_dev, depth, side), lambda s, *refs: (s, 0, 0)),
            pl.BlockSpec((depth_out, side, width), lambda s, *refs: (0, 0, 0)),
        ],
        scratch_shapes=[
            *apply_scratch(rows, blocks_dev, spread, depth, side, width),
            pltpu.VMEM((ring, 2, depth, depth), jnp.bfloat16),
            pltpu.VMEM((ring, depth, side), jnp.bfloat16),
            pltpu.VMEM((ring, side, width), jnp.bfloat16),
            pltpu.SemaphoreType.DMA((ring, 4)),
        ],
    )
    return pl.pallas_call(
        functools.partial(build_kernel, blocks_dev, spread),
        grid_spec=grid_spec,
        out_shape=[
            jax.ShapeDtypeStruct((2 * spread, depth, side), jnp.bfloat16),
            jax.ShapeDtypeStruct((depth_out, side, width), jnp.float32),
        ],
        compiler_params=pltpu.CompilerParams(vmem_limit_bytes=49 * 1024 * 1024),
        name="project_and_apply",
    )(in_slots, *tables, packed_a, packed_b, packed_i)


def apply_again(tables, projected, pieces, packed_a, blocks_dev):
    rows = packed_a.shape[0]
    _, depth, side = projected.shape
    cols, _, width = pieces.shape
    spread, depth_out = cols * blocks_dev, rows * blocks_dev
    grid_spec = pltpu.PrefetchScalarGridSpec(
        num_scalar_prefetch=3,
        grid=(spread // apply_group,),
        in_specs=[
            pl.BlockSpec(memory_space=pltpu.HBM),
            pl.BlockSpec(pieces.shape, lambda s, *refs: (0, 0, 0)),
            pl.BlockSpec(memory_space=pltpu.HBM),
        ],
        out_specs=pl.BlockSpec((depth_out, side, width), lambda s, *refs: (0, 0, 0)),
        scratch_shapes=[
            *apply_scratch(rows, blocks_dev, spread, depth, side, width),
            pltpu.VMEM(projected.shape, jnp.bfloat16),
            pltpu.SemaphoreType.DMA((spread // apply_group,)),
        ],
    )
    return pl.pallas_call(
        functools.partial(apply_kernel_body, blocks_dev, spread),
        grid_spec=grid_spec,
        out_shape=jax.ShapeDtypeStruct((depth_out, side, width), jnp.float32),
        compiler_params=pltpu.CompilerParams(vmem_limit_bytes=49 * 1024 * 1024),
        name="apply_again",
    )(*tables, projected, pieces, packed_a)


def on_device(
    vectors, energies, intersections, coarse, fine_coarse, coarse_slot, tile_codes, tile_count
):
    rows_count = lax.axis_size("row")
    cols_count = lax.axis_size("col")
    row_id = lax.axis_index("row")
    col_id = lax.axis_index("col")
    blocks_dev, pairs_coarse, tile_side = intersections.shape
    width_vec = vectors.shape[1]
    points_col = coarse.shape[0]
    spread = cols_count * blocks_dev
    depth_out = rows_count * blocks_dev
    groups_max = (tile_codes.shape[1] + (list_group - 1) * depth_out) // list_group
    index_out = jnp.arange(depth_out, dtype=jnp.int32)
    index_in = jnp.arange(spread, dtype=jnp.int32)
    out_blocks = (
        index_out // blocks_dev * cols_count + col_id
    ) * blocks_dev + index_out % blocks_dev
    in_blocks = (row_id * cols_count + index_in // blocks_dev) * blocks_dev + index_in % blocks_dev
    in_slots = lookup(coarse_slot, lookup(fine_coarse, in_blocks))
    out_points = lookup(fine_coarse, out_blocks) - col_id * points_col
    tables = list_tables(
        tile_codes[0], tile_count[0], depth_out, spread, out_points, groups_max
    )

    pair_energy = energies.reshape(-1, 1)
    across = jnp.swapaxes(intersections, 1, 2).reshape(-1, pairs_coarse)
    packed_a, packed_b, packed_i = gather_all(
        coarse[:, 0],
        across,
        jnp.concatenate(
            [intersections.reshape(-1, tile_side), vectors.astype(jnp.bfloat16)], axis=0
        ),
    )

    def linear(field):
        return pair_energy * field - spectrum_center * field

    def by_row(partial):
        return partial.reshape(rows_count, -1, width_vec)

    projected, partial = project_and_apply(
        in_slots, tables, packed_a, packed_b, packed_i, blocks_dev, tile_side
    )
    first_step, pieces = exchange(by_row(partial), linear(vectors), True)
    partial = apply_again(tables, projected, pieces, packed_a, blocks_dev)
    kernel_part = exchange(by_row(partial), vectors, False)
    second_step = 2.0 * ((linear(first_step) + kernel_part) / spectrum_half) - vectors
    return first_step, second_step


def solution(mesh):
    in_specs = (
        P(("row", "col"), None),
        P(("row", "col")),
        P(("row", "col"), None, None),
        P("col", "row", None, None),
        P(),
        P(),
        P(("row", "col"), None),
        P(("row", "col")),
    )
    out_specs = (P(("row", "col"), None), P(("row", "col"), None))
    return jax.shard_map(
        on_device, mesh=mesh, in_specs=in_specs, out_specs=out_specs, check_vma=False
    )
```
